32 devices in a mesh: grp: 2 (over x), patch: 16 (over z, y, core).
Axes of the slice: x: 2, y: 2, z: 4, core: 2. Of those that a mesh axis runs over, the one named last changes fastest.
Arguments:
- displace: float32 [2, 32768, 384], P('grp', 'patch'), may hold values from -6 to 6
- velocity: float32 [2, 32768, 384], P('grp', 'patch'), may hold values from -6 to 6
- ext_force: float32 [2, 32768, 384], P('grp', 'patch'), may hold values from -6 to 6
- inv_mass: float32 [2, 32768, 128], P('grp', 'patch'), may hold values from 0.1 to 6
- thickness: float32 [2, 32768, 128], P('grp', 'patch'), may hold values from 0.5 to 2
- stiff_bands: bfloat16 [5, 384, 384], replicated, may hold values from -0.125 to 0.125
- pair_points: int32 [2, 16, 3, 1536], P('grp', 'patch'), may hold values from 0 to 6143
- pair_weights: float32 [2, 16, 3, 1536], P('grp', 'patch'), may hold values from 0.25 to 1
Outputs:
- displace_new: float32 [2, 32768, 384], P('grp', 'patch')
- velocity_new: float32 [2, 32768, 384], P('grp', 'patch')
The draws below stay inside these ranges and needn't reach their ends.
Inputs may be any that keep to these rules, and one draw needn't show every extreme that they name: `pair_points`: entry e names the control point in row e // 3 of the sending block (rows counted within the block) and point e % 3 across the strip.
All inputs are finite; a program needn't handle non-finite values.
Results may differ from the reference program's by a relative error of at most 0.00094.
The reference program's roundings to bfloat16 on the way count: a program that leaves them out, or rounds other values in their place, can miss the bound.
Values may be sent and summed in bfloat16 or wider, within the bound.
A program may use at most 192 MiB of HBM per device.

```python
import math
import jax
import jax.numpy as jnp
from jax import lax

POINTS = 128
REACH = 2
SUBSTEPS = 4
TILES_DEV = 2048
SLOTS = 1536
ROW = 384
EDGE = 3
TILES = 32768
N_PATCH = 16


def draw_inv_mass(key, part):
    key_base, key_block, key_point = jax.random.split(jax.random.fold_in(key, 7), 3)
    block_total = 2 * N_PATCH
    position = jnp.arange(block_total, dtype=jnp.float32) / (block_total - 1)
    jitter = jax.random.uniform(key_block, (block_total,), jnp.float32, -0.05, 0.05)
    start = jax.random.uniform(key_base, (), jnp.float32, math.log(1.2), math.log(1.6))
    ceiling = jnp.exp(start + position * math.log(3.0) + jitter)
    per_row = jnp.repeat(ceiling.reshape(2, N_PATCH), TILES_DEV, axis=1)
    falling = jax.random.uniform(key_point, (2, TILES_DEV * N_PATCH, POINTS), jnp.float32, 0.0, math.log(4.0))
    return (per_row[:, :, None] * jnp.exp(-falling)).astype(jnp.float32)


def set_ends(drawn, rng, low, top_value):
    dims = drawn.shape
    place = [jax.random.randint(jax.random.fold_in(rng, axis), (), 0, dims[axis]) for axis in range(len(dims))]
    drawn = drawn.at[tuple(place)].set(low)
    longest = dims.index(max(dims))
    place[longest] = (place[longest] + 1) % dims[longest]
    return drawn.at[tuple(place)].set(top_value)


def block_scale(own_key, extent, cuts, low, top_value):
    loudness = 1.0
    for dim, shards_of in cuts:
        draws = jax.random.uniform(jax.random.fold_in(jax.random.fold_in(own_key, 6), dim), (shards_of,), jnp.float32, low / len(cuts), top_value / len(cuts))
        loudness = loudness * jnp.repeat(jnp.exp(draws), extent[dim] // shards_of).reshape((-1,) + (1,) * (len(extent) - 1 - dim))
    return loudness


def noise(key, shape, scale, limit, pieces=(), held_as=jnp.bfloat16):
    loudness = block_scale(key, shape, pieces, -0.22, 0.18) if pieces else 1.0
    array = jax.random.normal(key, shape, jnp.float32) * scale * loudness
    return jnp.minimum(jnp.maximum(array, -limit), limit).astype(held_as)


def setup_inputs(seed: int = 0) -> dict:
    seeds = jax.random.split(jax.random.key(seed), 9)
    displace = noise(seeds[0], (2, TILES, ROW), 1.0, 6.0, ((0, 2), (1, 16)), jnp.float32)
    velocity = noise(seeds[1], (2, TILES, ROW), 1.0, 6.0, ((0, 2), (1, 16)), jnp.float32)
    ext_force = noise(seeds[2], (2, TILES, ROW), 1.0, 6.0, ((0, 2), (1, 16)), jnp.float32)
    inv_mass = draw_inv_mass(jax.random.fold_in(seeds[8], 71), 0)
    thickness = jnp.clip(jnp.exp(math.log(2.0) - 1.3862944 * jax.random.uniform(seeds[4], (2, TILES, POINTS), jnp.float32) ** block_scale(seeds[4], (2, TILES, POINTS), ((0, 2), (1, 16)), -0.2, 0.2)), 0.5, 2.0)
    stiff_bands = noise(seeds[5], (2 * REACH + 1, ROW, ROW), ((2 * REACH + 1) * ROW) ** -0.5, 0.125)
    pair_points = set_ends(jax.random.randint(seeds[6], (2, N_PATCH, 3, SLOTS), 0, TILES_DEV * EDGE), jax.random.fold_in(seeds[6], 1), 0, (TILES_DEV * EDGE) - 1).astype(jnp.int32)
    pair_weights = jnp.clip(jnp.exp(math.log(1.0) - 1.3862944 * jax.random.uniform(seeds[7], (2, N_PATCH, 3, SLOTS), jnp.float32) ** block_scale(seeds[7], (2, N_PATCH, 3, SLOTS), ((0, 2), (1, 16)), -0.2, 0.2)), 0.25, 1.0)
    return dict(displace=displace, velocity=velocity, ext_force=ext_force, inv_mass=inv_mass, thickness=thickness, stiff_bands=stiff_bands, pair_points=pair_points, pair_weights=pair_weights)


PENALTY = 1.0
DAMPING = 0.5
COURANT = 0.4

def band_force(field, thickness, stiff_bands):
    row_count = field.shape[0]
    operand = lax.optimization_barrier(field.astype(jnp.bfloat16)).astype(jnp.float32)
    padded = jnp.pad(operand, ((REACH, REACH), (0, 0)))
    summed = jnp.zeros((row_count, 3 * POINTS), jnp.float32)
    for band_index in range(2 * REACH + 1):
        summed = summed + jnp.dot(padded[band_index:band_index + row_count], stiff_bands[band_index].astype(jnp.float32), precision=lax.Precision.HIGHEST)
    return (summed.reshape(row_count, 3, POINTS) * thickness[:, None, :]).reshape(row_count, 3 * POINTS)

def reference(displace, velocity, ext_force, inv_mass, thickness, stiff_bands, pair_points, pair_weights):
    row_width = 3 * POINTS
    base_step = COURANT * jnp.min(1.0 / jnp.sqrt(inv_mass * thickness))
    forces = [band_force(displace[group_index], thickness[group_index], stiff_bands) for group_index in range(2)]
    patch_base = (jnp.arange(N_PATCH, dtype=jnp.int32) * (TILES_DEV * row_width))[:, None, None]
    comp_offset = (jnp.arange(3, dtype=jnp.int32) * POINTS)[:, None, None, None]
    traces = []
    indices = []
    for group_index in range(2):
        pair_table = pair_points[group_index]
        flat_index = patch_base + pair_table // EDGE * row_width + pair_table % EDGE
        flat_index = (flat_index[None] + comp_offset).astype(jnp.int32)
        gathered = jnp.stack([displace[group_index].reshape(-1)[flat_index], velocity[group_index].reshape(-1)[flat_index], forces[group_index].reshape(-1)[flat_index]])
        traces.append(gathered)
        indices.append(flat_index)
    neighbour = (jnp.arange(N_PATCH, dtype=jnp.int32)[:, None] + jnp.arange(3, dtype=jnp.int32)[None, :] - 1).astype(jnp.int32)
    present = ((neighbour >= 0) & (neighbour < N_PATCH)).astype(jnp.float32)
    clipped = jnp.clip(neighbour, 0, N_PATCH - 1).astype(jnp.int32)
    mirror = jnp.broadcast_to((2 - jnp.arange(3, dtype=jnp.int32))[None, :], (N_PATCH, 3)).astype(jnp.int32)
    results_disp = []
    results_vel = []
    for group_index in range(2):
        gathered = traces[group_index]
        partner = traces[1 - group_index][:, :, clipped, mirror, :]
        weight = pair_weights[group_index] * present[:, :, None]
        slot_force = weight[None] * (-PENALTY * (gathered[0] - partner[0]) - DAMPING * (gathered[1] - partner[1]) + 0.5 * (partner[2] - gathered[2]))
        coupling = jnp.zeros((TILES * row_width,), jnp.float32).at[indices[group_index].reshape(-1)].add(slot_force.reshape(-1)).reshape(TILES, row_width)
        field = displace[group_index]
        moving = velocity[group_index]
        if group_index == 0:
            step_count = 1
            step_size = SUBSTEPS * base_step
        else:
            step_count = SUBSTEPS
            step_size = base_step
        for substep in range(step_count):
            if substep == 0:
                inner_force = forces[group_index]
            else:
                inner_force = band_force(field, thickness[group_index], stiff_bands)
            accel_now = ((ext_force[group_index] + coupling - inner_force).reshape(TILES, 3, POINTS) * inv_mass[group_index][:, None, :]).reshape(TILES, row_width)
            moving = moving + step_size * accel_now
            field = field + step_size * moving
        results_disp.append(field)
        results_vel.append(moving)
    return (jnp.stack(results_disp), jnp.stack(results_vel))
```

```python
import functools

import jax
import jax.numpy as jnp
from jax import lax
from jax.experimental import pallas as pl
from jax.experimental.pallas import tpu as pltpu
from jax.sharding import PartitionSpec as P

POINTS = 128
REACH = 2
SUBSTEPS = 4
EDGE = 3
COURANT = 0.4
HALO = REACH * SUBSTEPS
BASE = 2 * HALO
LANES = 128
COMPS = 3
SEG = 16
OFF = 8
INNER = 4
CODES = 32
LOW = 256
F32 = jnp.float32
BF16 = jnp.bfloat16
MESH = pl.DeviceIdType.MESH


def iota(shape, dim):
    return lax.broadcasted_iota(jnp.int32, shape, dim)


def dot(a, b):
    return jnp.dot(a, b, preferred_element_type=F32)


def dot_t(a, b):
    return lax.dot_general(a, b, (((1,), (1,)), ((), ())), preferred_element_type=F32)


def split_even(total, parts):
    base, extra = divmod(total, parts)
    sizes = [base + (i < extra) for i in range(parts)]
    return [(sum(sizes[:i]), n) for i, n in enumerate(sizes)]


def pair_force(xb, band, band_mid, first, n):
    width = xb.shape[3]
    taps = [
        xb[pl.ds(first + (r - REACH) // 2 + 1, n), r % 2].reshape(n * SEG, width)
        for r in range(2 * REACH + 2)
    ]
    lhs = jnp.concatenate(taps, axis=1)
    span = (2 * REACH + 1) * width
    low = dot(lhs[:, :span], band[:, : 2 * LANES])
    mid = dot(lhs, band_mid[...])
    high = dot(lhs[:, width:], band[:, LANES:])
    even = jnp.concatenate([low, mid[:, :LANES]], axis=1)
    odd = jnp.concatenate([mid[:, LANES:], high], axis=1)
    return even.reshape(n, SEG, width), odd.reshape(n, SEG, width)


def rows_of(ref, seg_len, j):
    return jnp.concatenate(
        [ref[pl.ds(OFF + j + half * 8 * seg_len, 8, stride=seg_len), :] for half in range(2)], axis=0
    )


def wide_rows_of(ref, seg_len, j):
    return jnp.concatenate([rows_of(ref.at[c], seg_len, j) for c in range(COMPS)], axis=1)


def three(a):
    return jnp.concatenate([a, a, a], axis=-1)


def kernel(
    n_grp,
    n_patch,
    disp_hbm,
    vel_hbm,
    ext_hbm,
    mass_hbm,
    thick_hbm,
    band_hbm,
    pts_hbm,
    wts_hbm,
    xo,
    wo,
    ao,
    co,
    xb1,
    band,
    band_mid,
    size_out,
    xs,
    vs,
    es,
    ms,
    ts,
    xb0,
    sbuf,
    dd,
    mixm,
    table,
    hot,
    place,
    pts,
    wts,
    code_ref,
    wl,
    own,
    sent,
    got,
    values,
    acc,
    far_src,
    far_dst,
    peak1,
    peak2,
    load_sem,
    halo_send,
    halo_recv,
    trace_send,
    trace_recv,
    far_send,
    far_recv,
    peak_send,
    peak_recv,
):
    g = lax.axis_index("grp")
    p = lax.axis_index("patch")
    rows = disp_hbm.shape[1]
    width = disp_hbm.shape[2]
    slots = pts_hbm.shape[3]
    total = rows + 2 * BASE
    seg_len = total // SEG
    pairs = seg_len // 2
    blocks = -(-seg_len // SEG)
    start = OFF + BASE
    own_rows = pl.ds(start, rows)
    has_low = p > 0
    has_high = p < n_patch - 1
    lanes = [pl.ds(c * LANES, LANES) for c in range(COMPS)]
    span = (2 * REACH + 1) * width

    def load(src, dst, k):
        return pltpu.make_async_copy(src, dst, load_sem.at[k])

    loads = {
        "pts": [load(pts_hbm.at[0, 0], pts, 0), load(wts_hbm.at[0, 0], wts, 1)],
        "x": [load(disp_hbm.at[0, :, lanes[c]], xs.at[c, own_rows], 2 + c) for c in range(COMPS)],
        "band": [
            load(band_hbm, band, 5),
            load(band_hbm.at[:, lanes[2]], band_mid.at[pl.ds(0, span), lanes[0]], 6),
            load(band_hbm.at[:, lanes[0]], band_mid.at[pl.ds(width, span), lanes[1]], 7),
        ],
        "t": [load(thick_hbm.at[0], ts.at[own_rows], 8)],
        "v": [load(vel_hbm.at[0, :, lanes[c]], vs.at[c, own_rows], 9 + c) for c in range(COMPS)],
        "m": [load(mass_hbm.at[0], ms.at[own_rows], 12)],
        "e": [load(ext_hbm.at[0, :, lanes[c]], es.at[c, own_rows], 13 + c) for c in range(COMPS)],
    }
    for group in loads.values():
        for copy in group:
            copy.start()

    def wait(*names):
        for name in names:
            for copy in loads[name]:
                copy.wait()

    inner = n_grp * INNER
    outer = n_patch // INNER
    mine_in = g * INNER + p % INNER
    mine_out = p // INNER

    def inner_id(k):
        to = (mine_in + k) % inner
        return {"grp": to // INNER, "patch": mine_out * INNER + to % INNER}

    def outer_id(k):
        return {"grp": g, "patch": (mine_out + k) % outer * INNER + p % INNER}

    barrier = pltpu.get_barrier_semaphore()

    def greet(device_id):
        pl.semaphore_signal(barrier, inc=1, device_id=device_id, device_id_type=MESH)

    for k in range(1, inner):
        greet(inner_id(k))
    for k in range(1, outer):
        greet(outer_id(k))

    @pl.when(has_low)
    def _():
        for to in (g, 1 - g):
            greet({"grp": to, "patch": p - 1})

    @pl.when(has_high)
    def _():
        for to in (g, 1 - g):
            greet({"grp": to, "patch": p + 1})

    def zero_rows(at, n):
        for ref in (xs, vs, es):
            for c in range(COMPS):
                ref[c, pl.ds(at, n), :] = jnp.zeros((n, LANES), F32)
        for ref in (ms, ts):
            ref[pl.ds(at, n), :] = jnp.zeros((n, LANES), F32)

    zero_rows(0, start - HALO)
    zero_rows(start + rows + HALO, start - HALO)
    pl.when(p == 0)(lambda: zero_rows(start - HALO, HALO))
    pl.when(p == n_patch - 1)(lambda: zero_rows(start + rows, HALO))
    band_mid[pl.ds(span, width), lanes[0]] = jnp.zeros((width, LANES), BF16)
    band_mid[pl.ds(0, width), lanes[1]] = jnp.zeros((width, LANES), BF16)
    for c in range(seg_len * SEG, blocks * LOW, SEG):
        mixm[pl.ds(c, SEG), :] = jnp.zeros((SEG, LANES), BF16)

    wait("pts")
    entry = pts[...]
    row = entry // EDGE
    point = entry - row * EDGE
    row = row + BASE
    seg = row // seg_len
    j_row = row - seg * seg_len
    block = j_row // SEG
    code_ref[...] = block * EDGE + point
    pts[...] = (j_row - block * SEG) * SEG + seg
    third = slots // 3
    parts = [pl.ds(q * third, third) for q in range(3)]
    low_id = iota((LOW, third), 0)
    row16 = iota((SEG, third), 0)
    exists = (has_low, None, has_high)
    for j in range(3):
        weight = jnp.zeros((SEG, third), F32)
        for q in range(3):
            low = pts[pl.ds(j, 1), parts[q]]
            hot[j, :, parts[q]] = jnp.where(low_id == low, 1.0, 0.0).astype(BF16)
            weight = jnp.where(row16 % 3 == q, wts[pl.ds(j, 1), parts[q]], weight)
        present = 1.0 if exists[j] is None else jnp.where(exists[j], 1.0, 0.0)
        wl[j] = jnp.where(row16 < 3 * COMPS, weight * present, 0.0)

    place_row = iota((LOW, width), 0) % LANES
    place_lane = iota((LOW, width), 1)
    comp_row = place_row // CODES
    code_row = place_row % CODES
    hit = (comp_row == place_lane // POINTS) & (code_row % EDGE == place_lane % POINTS)
    for h in range(blocks):
        place[h] = jnp.where(hit & (code_row // EDGE == h), 1.0, 0.0).astype(BF16)

    @pl.when(p == 0)
    def _():
        got[0] = jnp.zeros(got.shape[1:], BF16)

    @pl.when(p == n_patch - 1)
    def _():
        got[2] = jnp.zeros(got.shape[1:], BF16)

    def halo_copies(name, up):
        src = pl.ds(rows - HALO, HALO) if up else pl.ds(0, HALO)
        dst = pl.ds(start - HALO, HALO) if up else pl.ds(start + rows, HALO)
        to = p + 1 if up else p - 1
        source, target, k = {
            "x": (disp_hbm, xs, 0),
            "v": (vel_hbm, vs, 3),
            "e": (ext_hbm, es, 6),
            "m": (mass_hbm, ms, 9),
            "t": (thick_hbm, ts, 10),
        }[name]
        if name in "xve":
            refs = [(source.at[0, src, lanes[c]], target.at[c, dst]) for c in range(COMPS)]
        else:
            refs = [(source.at[0, src], target.at[dst])]
        return [
            pltpu.make_async_remote_copy(
                src_ref=a,
                dst_ref=b,
                send_sem=halo_send.at[k + i, int(up)],
                recv_sem=halo_recv.at[k + i, int(up)],
                device_id={"grp": g, "patch": to},
                device_id_type=MESH,
            )
            for i, (a, b) in enumerate(refs)
        ]

    def wait_halo(*names):
        @pl.when(has_low)
        def _():
            for name in names:
                for copy in halo_copies(name, True):
                    copy.wait_recv()

        @pl.when(has_high)
        def _():
            for name in names:
                for copy in halo_copies(name, False):
                    copy.wait_recv()

    more = 2 * has_low.astype(jnp.int32) + 2 * has_high.astype(jnp.int32)
    pl.semaphore_wait(barrier, inner + outer - 2 + more)

    @pl.when(has_high)
    def _():
        for name in "xtvme":
            for copy in halo_copies(name, True):
                copy.start()

    @pl.when(has_low)
    def _():
        for name in "xtvme":
            for copy in halo_copies(name, False):
                copy.start()

    def pack(first, n):
        for i in range(first, first + n):
            for par in range(2):
                xb0[i + 1, par] = wide_rows_of(xs, seg_len, 2 * i + par).astype(BF16)

    lane = iota((SEG, LANES), 1)

    def mix_rows(first, n):
        for i in range(first, first + n):
            for par in range(2):
                j = 2 * i + par
                thick = rows_of(ts, seg_len, j)
                mixed = []
                for c in range(COMPS):
                    f = thick * sbuf[i, par, :, lanes[c]]
                    mixed.append(
                        rows_of(xs.at[c], seg_len, j) + 0.5 * (rows_of(vs.at[c], seg_len, j) + f)
                    )
                out = jnp.where(lane < 3, mixed[0], 0.0)
                out = jnp.where((lane >= 3) & (lane < 6), pltpu.roll(mixed[1], 3, 1), out)
                out = jnp.where((lane >= 6) & (lane < 9), pltpu.roll(mixed[2], 6, 1), out)
                mixm[pl.ds(j * SEG, SEG), :] = out.astype(BF16)

    def first_force(first, n):
        even, odd = pair_force(xb0, band, band_mid, first, n)
        sbuf[pl.ds(first, n), 0] = even
        sbuf[pl.ds(first, n), 1] = odd

    chunks = split_even(pairs, 4)
    middle = (chunks[1][0] - 1, chunks[1][1] + chunks[2][1] + 2)
    wait("x", "band")
    pack(*middle)
    first_force(*chunks[1])
    first_force(*chunks[2])
    wait("t", "v", "m")
    top_rows = 256
    high = jnp.zeros((8, LANES), F32)

    def peak_step(i, high):
        at = pl.ds(pl.multiple_of(start + i * top_rows, 8), top_rows)
        product = (ms[at, :] * ts[at, :]).reshape(top_rows // 8, 8, LANES)
        return jnp.maximum(high, jnp.max(product, axis=0))

    peak1[0] = lax.fori_loop(0, rows // top_rows, peak_step, high)

    def peak_copy(ref, k, to, phase):
        return pltpu.make_async_remote_copy(
            src_ref=ref.at[0],
            dst_ref=ref.at[k],
            send_sem=peak_send.at[phase],
            recv_sem=peak_recv.at[phase],
            device_id=to,
            device_id_type=MESH,
        )

    for k in range(1, inner):
        peak_copy(peak1, k, inner_id(k), 0).start()
    wait_halo("x", "t", "v")
    pack(-1, middle[0] + 1)
    pack(sum(middle), pairs + 1 - sum(middle))
    first_force(*chunks[0])
    mix_rows(*chunks[1])
    mix_rows(*chunks[2])
    first_force(*chunks[3])
    mix_rows(*chunks[0])
    mix_rows(*chunks[3])

    arrived1 = peak1.at[pl.ds(1, inner - 1)]
    pltpu.make_async_copy(arrived1, arrived1, peak_recv.at[0]).wait()
    peak2[0] = jnp.max(peak1[...], axis=0)
    for k in range(1, outer):
        peak_copy(peak2, k, outer_id(k), 1).start()

    pick_row = iota((COMPS * CODES, LANES), 0)
    pick_lane = iota((COMPS * CODES, LANES), 1)
    comp_of = pick_row // CODES
    code_of = pick_row % CODES
    picked = (pick_lane == comp_of * EDGE + code_of % EDGE) & (pick_lane < COMPS * EDGE)
    found_table = jnp.zeros((COMPS * CODES, LOW), F32)
    for h in range(blocks):
        pick = jnp.where(picked & (code_of // EDGE == h), 1.0, 0.0).astype(BF16)
        found_table += dot_t(pick, mixm[pl.ds(h * LOW, LOW), :])
    table[...] = found_table.astype(BF16)

    def trace_copy(j):
        return pltpu.make_async_remote_copy(
            src_ref=sent.at[j],
            dst_ref=got.at[2 - j],
            send_sem=trace_send.at[j],
            recv_sem=trace_recv.at[2 - j],
            device_id={"grp": 1 - g, "patch": p + (j - 1)},
            device_id_type=MESH,
        )

    def guarded(cond, run):
        if cond is None:
            run()
        else:
            pl.when(cond)(run)

    code_id = iota((CODES, third), 0)

    for j in (0, 2, 1):
        result = jnp.zeros((SEG, third), F32)
        for q in range(3):
            found = dot(table[...], hot[j, :, parts[q]])
            mask = code_id == code_ref[pl.ds(j, 1), parts[q]]
            for c in range(COMPS):
                chosen = jnp.where(mask, found[c * CODES : (c + 1) * CODES], 0.0)
                result = jnp.where(
                    row16 == c * 3 + q, jnp.sum(chosen, axis=0, keepdims=True), result
                )
        own[j] = result
        sent[j] = result.astype(BF16)
        guarded(exists[j], lambda j=j: trace_copy(j).start())

    arrived2 = peak2.at[pl.ds(1, outer - 1)]
    pltpu.make_async_copy(arrived2, arrived2, peak_recv.at[1]).wait()
    top = jnp.max(jnp.max(peak2[...], axis=0), axis=(0, 1), keepdims=True)
    base_step = COURANT * (1.0 / jnp.sqrt(top))
    size = jnp.where(g == 0, SUBSTEPS * base_step, base_step)
    square = size * size
    wait("e")
    wait_halo("m", "e")

    def prepare(i, carry):
        for k in range(10):
            j = i * 10 + k
            at = (i * 5 + k // 2, k % 2)
            mass = square * rows_of(ms, seg_len, j)
            coef = mass * rows_of(ts, seg_len, j)
            applied = three(mass) * wide_rows_of(es, seg_len, j)
            moved = size * wide_rows_of(vs, seg_len, j) + (applied - three(coef) * sbuf[at])
            ao[at] = applied
            co[at] = coef
            dd[at] = mass
            wo[at] = moved
            xo[at] = wide_rows_of(xs, seg_len, j)
        return carry

    lax.fori_loop(0, seg_len // 10, prepare, 0)

    for step, j in enumerate((1, 0, 2)):
        guarded(exists[j], lambda j=j: trace_copy(2 - j).wait_recv())
        value = (got[j].astype(F32) - own[j]) * wl[j]
        coarse = value.astype(BF16).astype(F32)
        fine = value - coarse
        for q in range(3):
            mask = code_id == code_ref[pl.ds(j, 1), parts[q]]
            zero = jnp.zeros((CODES, third), BF16)
            stack = []
            for piece in (coarse, fine):
                for c in range(COMPS):
                    one = piece[c * 3 + q : c * 3 + q + 1]
                    stack.append(jnp.where(mask, one, 0.0).astype(BF16))
                stack.append(zero)
            values[:, parts[q]] = jnp.concatenate(stack, axis=0)
        summed = dot_t(hot[j], values[...])
        if step == 0:
            acc[...] = summed
        else:
            acc[...] += summed

    both = acc[:, :LANES] + acc[:, LANES:]
    acc[:, :LANES] = both
    first = both.astype(BF16)
    pieces = jnp.concatenate([first, (both - first.astype(F32)).astype(BF16)], axis=1)

    fine_group = g == 1

    def edge_lane_rows(first_row):
        out = []
        for k in range(HALO):
            j = (first_row + k + BASE) % seg_len
            s = (first_row + k + BASE) // seg_len
            one = acc[pl.ds((j % SEG) * SEG + s, 1), lanes[0]]
            keep = iota((1, LANES), 1) % CODES // EDGE == j // SEG
            out.append(jnp.where(keep, one, 0.0))
        return jnp.concatenate(out, axis=0)

    far_src[0] = edge_lane_rows(0)
    far_src[1] = edge_lane_rows(rows - HALO)

    def far_copy(up):
        return pltpu.make_async_remote_copy(
            src_ref=far_src.at[int(up)],
            dst_ref=far_dst.at[1 - int(up)],
            send_sem=far_send.at[int(up)],
            recv_sem=far_recv.at[int(up)],
            device_id={"grp": g, "patch": p + 1 if up else p - 1},
            device_id_type=MESH,
        )

    pl.when(jnp.logical_not(fine_group & has_low))(
        lambda: far_dst.at[0].__setitem__(..., jnp.zeros((HALO, LANES), F32))
    )
    pl.when(jnp.logical_not(fine_group & has_high))(
        lambda: far_dst.at[1].__setitem__(..., jnp.zeros((HALO, LANES), F32))
    )
    pl.when(fine_group & has_high)(lambda: far_copy(True).start())
    pl.when(fine_group & has_low)(lambda: far_copy(False).start())

    half = SEG // 2

    def finish(h):
        n = min(half, pairs - h * half)
        placed = dot(pieces[: 2 * n * SEG], place[h]).reshape(n, 2, SEG, width)
        for k in range(n):
            for par in range(2):
                at = (h * half + k, par)
                extra = three(dd[at]) * placed[k, par]
                moved = wo[at] + extra
                there = xo[at] + moved
                ao[at] = ao[at] + extra
                wo[at] = moved
                xo[at] = there
                xb1[at[0] + 1, par] = there.astype(BF16)

    for h in range(blocks):
        finish(h)

    pl.when(fine_group & has_low)(lambda: far_copy(True).wait_recv())
    pl.when(fine_group & has_high)(lambda: far_copy(False).wait_recv())
    any_place = place[0]
    for h in range(1, blocks):
        any_place = any_place + place[h]
    far = far_dst[...].reshape(2 * HALO, LANES)
    far_first = far.astype(BF16)
    far_pieces = jnp.concatenate([far_first, (far - far_first.astype(F32)).astype(BF16)], axis=1)
    far_placed = dot(far_pieces, any_place)
    seg_id = iota((SEG, width), 0)
    for side, first_row in ((0, -HALO), (1, rows)):
        for k in range(HALO):
            j = (first_row + k + BASE) % seg_len
            s = (first_row + k + BASE) // seg_len
            at = (j // 2, j % 2)
            one = far_placed[side * HALO + k : side * HALO + k + 1]
            extra = three(dd[at]) * jnp.where(seg_id == s, one, 0.0)
            there = xo[at] + extra
            ao[at] = ao[at] + extra
            wo[at] = wo[at] + extra
            xo[at] = there
            xb1[at[0] + 1, at[1]] = there.astype(BF16)
    for par in range(2):
        xb1[0, par] = pltpu.roll(xo[pairs - 1, par], 1, 0).astype(BF16)
        xb1[pairs + 1, par] = pltpu.roll(xo[0, par], SEG - 1, 0).astype(BF16)
    size_out[...] = jnp.broadcast_to(1.0 / size, size_out.shape)

    @pl.when(has_high)
    def _():
        for name in "xtvme":
            for copy in halo_copies(name, True):
                copy.wait_send()

    @pl.when(has_low)
    def _():
        for name in "xtvme":
            for copy in halo_copies(name, False):
                copy.wait_send()

    for j in range(3):
        guarded(exists[j], lambda j=j: trace_copy(j).wait_send())
    pl.when(fine_group & has_high)(lambda: far_copy(True).wait_send())
    pl.when(fine_group & has_low)(lambda: far_copy(False).wait_send())
    pltpu.make_async_copy(arrived1, arrived1, peak_send.at[0]).wait()
    pltpu.make_async_copy(arrived2, arrived2, peak_send.at[1]).wait()


def steps_kernel(
    x1, w1, a, c, xb1, band, band_mid, inverse, disp_out, vel_out, xo, wo, xb2, xs, vs, out_sem
):
    g = lax.axis_index("grp")
    rows = disp_out.shape[1]
    width = disp_out.shape[2]
    total = rows + 2 * BASE
    seg_len = total // SEG
    pairs = seg_len // 2
    scale = inverse[0:1, 0:1]

    def put(i, par, x, w):
        j = 2 * i + par
        v = w * scale
        for value, ref in ((x, xs), (v, vs)):
            for c in range(COMPS):
                for half in range(2):
                    at = pl.ds(OFF + j + half * 8 * seg_len, 8, stride=seg_len)
                    ref[c, at, :] = value[half * 8 : half * 8 + 8, c * LANES : (c + 1) * LANES]

    def drain():
        copies = []
        for k, (ref, out) in enumerate(((xs, disp_out), (vs, vel_out))):
            for c in range(COMPS):
                copies.append(
                    pltpu.make_async_copy(
                        ref.at[c, pl.ds(OFF + BASE, rows)],
                        out.at[0, :, pl.ds(c * LANES, LANES)],
                        out_sem.at[k, c],
                    )
                )
        for copy in copies:
            copy.start()
        for copy in copies:
            copy.wait()

    @pl.when(g == 0)
    def _():
        def move(i, carry):
            for par in range(2):
                put(i, par, x1[i, par], w1[i, par])
            return carry

        lax.fori_loop(0, pairs, move, 0)
        drain()

    @pl.when(g == 1)
    def _():
        cur, nxt = xb1, xb2
        src_x, src_w = x1, w1
        for k in range(SUBSTEPS - 1):
            last = k == SUBSTEPS - 2
            for first, n in split_even(pairs, 4):
                here = pl.ds(first, n)
                for par, inner in enumerate(pair_force(cur, band, band_mid, first, n)):
                    w = src_w[here, par] + a[here, par] - three(c[here, par]) * inner
                    x = src_x[here, par] + w
                    if last:
                        for i in range(n):
                            put(first + i, par, x[i], w[i])
                    else:
                        wo[here, par] = w
                        xo[here, par] = x
                        nxt[pl.ds(first + 1, n), par] = x.astype(BF16)
            if not last:
                for par in range(2):
                    nxt[0, par] = pltpu.roll(xo[pairs - 1, par], 1, 0).astype(BF16)
                    nxt[pairs + 1, par] = pltpu.roll(xo[0, par], SEG - 1, 0).astype(BF16)
            cur, nxt = nxt, cur
            src_x, src_w = xo, wo
        drain()


def per_device(
    n_grp,
    n_patch,
    displace,
    velocity,
    ext_force,
    inv_mass,
    thickness,
    stiff_bands,
    pair_points,
    pair_weights,
):
    rows, width = displace.shape[1:]
    slots = pair_points.shape[3]
    total = rows + 2 * BASE
    seg_len = total // SEG
    pairs = seg_len // 2
    blocks = -(-seg_len // SEG)
    third = slots // 3
    taps = stiff_bands.shape[0]
    bands = stiff_bands.reshape(taps * width, width)
    hbm = pl.BlockSpec(memory_space=pltpu.HBM)
    vmem = pl.BlockSpec(memory_space=pltpu.VMEM)
    dma = pltpu.SemaphoreType.DMA
    lined = total + 2 * OFF
    wide = pltpu.VMEM((COMPS, lined, LANES), F32)
    slim = pltpu.VMEM((lined, LANES), F32)
    seg_wide = pltpu.VMEM((pairs, 2, SEG, width), F32)
    seg_slim = pltpu.VMEM((pairs, 2, SEG, LANES), F32)
    seg_bf16 = pltpu.VMEM((pairs + 2, 2, SEG, width), BF16)
    state = pl.pallas_call(
        functools.partial(kernel, n_grp, n_patch),
        out_shape=[
            seg_wide,
            seg_wide,
            seg_wide,
            seg_slim,
            seg_bf16,
            pltpu.VMEM(bands.shape, BF16),
            pltpu.VMEM(((taps + 1) * width, 2 * LANES), BF16),
            pltpu.VMEM((8, LANES), F32),
        ],
        in_specs=[hbm] * 8,
        out_specs=[vmem] * 8,
        scratch_shapes=[
            wide,
            wide,
            wide,
            slim,
            slim,
            seg_bf16,
            seg_wide,
            seg_slim,
            pltpu.VMEM((blocks * LOW, LANES), BF16),
            pltpu.VMEM((COMPS * CODES, LOW), BF16),
            pltpu.VMEM((3, LOW, slots), BF16),
            pltpu.VMEM((blocks, LOW, width), BF16),
            pltpu.VMEM((3, slots), jnp.int32),
            pltpu.VMEM((3, slots), F32),
            pltpu.VMEM((3, slots), jnp.int32),
            pltpu.VMEM((3, SEG, third), F32),
            pltpu.VMEM((3, SEG, third), F32),
            pltpu.VMEM((3, SEG, third), BF16),
            pltpu.VMEM((3, SEG, third), BF16),
            pltpu.VMEM((LOW, slots), BF16),
            pltpu.VMEM((LOW, LOW), F32),
            pltpu.VMEM((2, HALO, LANES), F32),
            pltpu.VMEM((2, HALO, LANES), F32),
            pltpu.VMEM((n_grp * INNER, 8, LANES), F32),
            pltpu.VMEM((n_patch // INNER, 8, LANES), F32),
            dma((16,)),
            dma((11, 2)),
            dma((11, 2)),
            dma((3,)),
            dma((3,)),
            dma((2,)),
            dma((2,)),
            dma((2,)),
            dma((2,)),
        ],
        compiler_params=pltpu.CompilerParams(
            has_side_effects=True, collective_id=0, vmem_limit_bytes=44 * 1024 * 1024
        ),
        name="couple_step",
    )(displace, velocity, ext_force, inv_mass, thickness, bands, pair_points, pair_weights)
    return pl.pallas_call(
        steps_kernel,
        out_shape=[jax.ShapeDtypeStruct(displace.shape, F32)] * 2,
        in_specs=[vmem] * 8,
        out_specs=[hbm] * 2,
        scratch_shapes=[seg_wide, seg_wide, seg_bf16, wide, wide, dma((2, COMPS))],
        compiler_params=pltpu.CompilerParams(vmem_limit_bytes=34 * 1024 * 1024),
        name="fine_steps",
    )(*state)


def solution(mesh):
    return jax.shard_map(
        functools.partial(per_device, mesh.shape["grp"], mesh.shape["patch"]),
        mesh=mesh,
        in_specs=(
            P("grp", "patch", None),
            P("grp", "patch", None),
            P("grp", "patch", None),
            P("grp", "patch", None),
            P("grp", "patch", None),
            P(),
            P("grp", "patch", None, None),
            P("grp", "patch", None, None),
        ),
        out_specs=(P("grp", "patch", None), P("grp", "patch", None)),
        check_vma=False,
    )
```

```python
import functools

import jax
import jax.numpy as jnp
from jax import lax
from jax.experimental import pallas as pl
from jax.experimental.pallas import tpu as pltpu
from jax.sharding import PartitionSpec as P

POINTS = 128
REACH = 2
SUBSTEPS = 4
EDGE = 3
COURANT = 0.4
HALO = REACH * SUBSTEPS
BASE = 2 * HALO
LANES = 128
COMPS = 3
SEG = 16
OFF = 8
INNER = 4
CODES = 32
LOW = 256
F32 = jnp.float32
BF16 = jnp.bfloat16
MESH = pl.DeviceIdType.MESH


def iota(shape, dim):
    return lax.broadcasted_iota(jnp.int32, shape, dim)


def dot(a, b):
    return jnp.dot(a, b, preferred_element_type=F32)


def dot_t(a, b):
    return lax.dot_general(a, b, (((1,), (1,)), ((), ())), preferred_element_type=F32)


def split_even(total, parts):
    base, extra = divmod(total, parts)
    sizes = [base + (i < extra) for i in range(parts)]
    return [(sum(sizes[:i]), n) for i, n in enumerate(sizes)]


def pair_force(xb, band, band_mid, *ranges):
    width = xb.shape[3]
    taps = []
    for r in range(2 * REACH + 2):
        got = [
            xb[pl.ds(first + (r - REACH) // 2 + 1, n), r % 2].reshape(n * SEG, width)
            for first, n in ranges
        ]
        taps.append(got[0] if len(got) == 1 else jnp.concatenate(got, axis=0))
    n = sum(n for _, n in ranges)
    lhs = jnp.concatenate(taps, axis=1)
    span = (2 * REACH + 1) * width
    low = dot(lhs[:, :span], band[:, : 2 * LANES])
    mid = dot(lhs, band_mid[...])
    high = dot(lhs[:, width:], band[:, LANES:])
    even = jnp.concatenate([low, mid[:, :LANES]], axis=1)
    odd = jnp.concatenate([mid[:, LANES:], high], axis=1)
    return even.reshape(n, SEG, width), odd.reshape(n, SEG, width)


def advance(sums, src, dst, a, c, nxt, *ranges):
    done = 0
    for first, n in ranges:
        here = pl.ds(first, n)
        for par in range(2):
            inner = sums[par][done : done + n]
            w = src[1][here, par] + a[here, par] - three(c[here, par]) * inner
            x = src[0][here, par] + w
            dst[0][here, par] = x
            dst[1][here, par] = w
            nxt[pl.ds(first + 1, n), par] = x.astype(BF16)
        done += n


def row_ranges(pairs):
    edge = (BASE + REACH) // 2
    chunks = [(edge + first, n) for first, n in split_even(pairs - 2 * edge, 3)]
    return edge, chunks, [(0, edge), (pairs - edge, edge)]


def rows_of(ref, seg_len, j):
    return jnp.concatenate(
        [ref[pl.ds(OFF + j + half * 8 * seg_len, 8, stride=seg_len), :] for half in range(2)], axis=0
    )


def wide_rows_of(ref, seg_len, j):
    return jnp.concatenate([rows_of(ref.at[c], seg_len, j) for c in range(COMPS)], axis=1)


def three(a):
    return jnp.concatenate([a, a, a], axis=-1)


def kernel(
    n_grp,
    n_patch,
    disp_hbm,
    vel_hbm,
    ext_hbm,
    mass_hbm,
    thick_hbm,
    band_hbm,
    pts_hbm,
    wts_hbm,
    xo,
    wo,
    ao,
    co,
    xb1,
    xb2,
    band,
    band_mid,
    size_out,
    xs,
    vs,
    es,
    ms,
    ts,
    xb0,
    sbuf,
    dd,
    mixm,
    table,
    hot,
    place,
    pts_in,
    pts,
    wts,
    code_ref,
    wl,
    own,
    sent,
    got,
    acc,
    far_src,
    far_dst,
    peak1,
    peak2,
    load_sem,
    halo_send,
    halo_recv,
    trace_send,
    trace_recv,
    far_send,
    far_recv,
    peak_send,
    peak_recv,
):
    g = lax.axis_index("grp")
    p = lax.axis_index("patch")
    rows = disp_hbm.shape[1]
    width = disp_hbm.shape[2]
    slots = pts_hbm.shape[2]
    total = rows + 2 * BASE
    seg_len = total // SEG
    pairs = seg_len // 2
    blocks = -(-seg_len // SEG)
    start = OFF + BASE
    own_rows = pl.ds(start, rows)
    has_low = p > 0
    has_high = p < n_patch - 1
    lanes = [pl.ds(c * LANES, LANES) for c in range(COMPS)]
    span = (2 * REACH + 1) * width

    def load(src, dst, k):
        return pltpu.make_async_copy(src, dst, load_sem.at[k])

    loads = {
        "pts": [load(pts_hbm, pts_in, 0), load(wts_hbm, wts, 1)],
        "x": [load(disp_hbm.at[0, :, lanes[c]], xs.at[c, own_rows], 2 + c) for c in range(COMPS)],
        "band": [
            load(band_hbm, band, 5),
            load(band_hbm.at[:, lanes[2]], band_mid.at[pl.ds(0, span), lanes[0]], 6),
            load(band_hbm.at[:, lanes[0]], band_mid.at[pl.ds(width, span), lanes[1]], 7),
        ],
        "t": [load(thick_hbm.at[0], ts.at[own_rows], 8)],
        "m": [load(mass_hbm.at[0], ms.at[own_rows], 12)],
        "v": [load(vel_hbm.at[0, :, lanes[c]], vs.at[c, own_rows], 9 + c) for c in range(COMPS)],
        "e": [load(ext_hbm.at[0, :, lanes[c]], es.at[c, own_rows], 13 + c) for c in range(COMPS)],
    }

    def begin(*names):
        for name in names:
            for copy in loads[name]:
                copy.start()

    begin("pts", "band", "x")

    def wait(*names):
        for name in names:
            for copy in loads[name]:
                copy.wait()

    inner = n_grp * INNER
    outer = n_patch // INNER
    mine_in = g * INNER + p % INNER
    mine_out = p // INNER

    def inner_id(k):
        to = (mine_in + k) % inner
        return {"grp": to // INNER, "patch": mine_out * INNER + to % INNER}

    def outer_id(k):
        return {"grp": g, "patch": (mine_out + k) % outer * INNER + p % INNER}

    barrier = pltpu.get_barrier_semaphore()

    def greet(device_id):
        pl.semaphore_signal(barrier, inc=1, device_id=device_id, device_id_type=MESH)

    for k in range(1, inner):
        greet(inner_id(k))
    for k in range(1, outer):
        greet(outer_id(k))

    @pl.when(has_low)
    def _():
        for to in (g, 1 - g):
            greet({"grp": to, "patch": p - 1})

    @pl.when(has_high)
    def _():
        for to in (g, 1 - g):
            greet({"grp": to, "patch": p + 1})

    def zero_rows(at, n):
        for ref in (xs, vs, es):
            for c in range(COMPS):
                ref[c, pl.ds(at, n), :] = jnp.zeros((n, LANES), F32)
        for ref in (ms, ts):
            ref[pl.ds(at, n), :] = jnp.zeros((n, LANES), F32)

    zero_rows(0, start - HALO)
    zero_rows(start + rows + HALO, start - HALO)
    pl.when(p == 0)(lambda: zero_rows(start - HALO, HALO))
    pl.when(p == n_patch - 1)(lambda: zero_rows(start + rows, HALO))
    band_mid[pl.ds(span, width), lanes[0]] = jnp.zeros((width, LANES), BF16)
    band_mid[pl.ds(0, width), lanes[1]] = jnp.zeros((width, LANES), BF16)
    for c in range(seg_len * SEG, blocks * LOW, SEG):
        mixm[pl.ds(c, SEG), :] = jnp.zeros((SEG, LANES), BF16)

    wait("pts")
    entry = pts_in[...].reshape(3, slots)
    row = entry // EDGE
    point = entry - row * EDGE
    row = row + BASE
    seg = row // seg_len
    j_row = row - seg * seg_len
    block = j_row // SEG
    code_ref[...] = block * EDGE + point
    pts[...] = (j_row - block * SEG) * SEG + seg
    third = slots // 3
    parts = [pl.ds(q * third, third) for q in range(3)]
    low_id = iota((LOW, third), 0)
    row16 = iota((SEG, third), 0)
    exists = (has_low, None, has_high)
    for j in range(3):
        weight = jnp.zeros((SEG, third), F32)
        for q in range(3):
            low = pts[pl.ds(j, 1), parts[q]]
            hot[j, :, parts[q]] = jnp.where(low_id == low, 1.0, 0.0).astype(BF16)
            weight = jnp.where(row16 % 3 == q, wts[j, :, parts[q]], weight)
        present = 1.0 if exists[j] is None else jnp.where(exists[j], 1.0, 0.0)
        wl[j] = jnp.where(row16 < 3 * COMPS, weight * present, 0.0)

    begin("t", "m", "v", "e")
    place_row = iota((LOW, width), 0) % LANES
    place_lane = iota((LOW, width), 1)
    comp_row = place_row // CODES
    code_row = place_row % CODES
    hit = (comp_row == place_lane // POINTS) & (code_row % EDGE == place_lane % POINTS)
    for h in range(blocks):
        place[h] = jnp.where(hit & (code_row // EDGE == h), 1.0, 0.0).astype(BF16)

    @pl.when(p == 0)
    def _():
        got[0] = jnp.zeros(got.shape[1:], BF16)

    @pl.when(p == n_patch - 1)
    def _():
        got[2] = jnp.zeros(got.shape[1:], BF16)

    def halo_copies(name, up):
        src = pl.ds(rows - HALO, HALO) if up else pl.ds(0, HALO)
        dst = pl.ds(start - HALO, HALO) if up else pl.ds(start + rows, HALO)
        to = p + 1 if up else p - 1
        source, target, k = {
            "x": (disp_hbm, xs, 0),
            "v": (vel_hbm, vs, 3),
            "e": (ext_hbm, es, 6),
            "m": (mass_hbm, ms, 9),
            "t": (thick_hbm, ts, 10),
        }[name]
        if name in "xve":
            refs = [(source.at[0, src, lanes[c]], target.at[c, dst]) for c in range(COMPS)]
        else:
            refs = [(source.at[0, src], target.at[dst])]
        return [
            pltpu.make_async_remote_copy(
                src_ref=a,
                dst_ref=b,
                send_sem=halo_send.at[k + i, int(up)],
                recv_sem=halo_recv.at[k + i, int(up)],
                device_id={"grp": g, "patch": to},
                device_id_type=MESH,
            )
            for i, (a, b) in enumerate(refs)
        ]

    def wait_halo(*names):
        @pl.when(has_low)
        def _():
            for name in names:
                for copy in halo_copies(name, True):
                    copy.wait_recv()

        @pl.when(has_high)
        def _():
            for name in names:
                for copy in halo_copies(name, False):
                    copy.wait_recv()

    def pack(first, n):
        for i in range(first, first + n):
            for par in range(2):
                xb0[i + 1, par] = wide_rows_of(xs, seg_len, 2 * i + par).astype(BF16)

    lane = iota((SEG, LANES), 1)

    def mix_rows(first, n):
        for i in range(first, first + n):
            for par in range(2):
                j = 2 * i + par
                thick = rows_of(ts, seg_len, j)
                mixed = []
                for c in range(COMPS):
                    f = thick * sbuf[i, par, :, lanes[c]]
                    mixed.append(
                        rows_of(xs.at[c], seg_len, j) + 0.5 * (rows_of(vs.at[c], seg_len, j) + f)
                    )
                out = jnp.where(lane < 3, mixed[0], 0.0)
                out = jnp.where((lane >= 3) & (lane < 6), pltpu.roll(mixed[1], 3, 1), out)
                out = jnp.where((lane >= 6) & (lane < 9), pltpu.roll(mixed[2], 6, 1), out)
                mixm[pl.ds(j * SEG, SEG), :] = out.astype(BF16)

    def first_force(*ranges):
        done = 0
        sums = pair_force(xb0, band, band_mid, *ranges)
        for first, n in ranges:
            for par in range(2):
                sbuf[pl.ds(first, n), par] = sums[par][done : done + n]
            done += n

    edge, chunks, edges = row_ranges(pairs)
    wait("x", "band")
    pack(edge - 1, pairs - 2 * edge + 2)
    first_force(chunks[0])
    wait("t", "m")
    top_rows = 256
    high = jnp.zeros((8, LANES), F32)

    def peak_step(i, high):
        at = pl.ds(pl.multiple_of(start + i * top_rows, 8), top_rows)
        product = (ms[at, :] * ts[at, :]).reshape(top_rows // 8, 8, LANES)
        return jnp.maximum(high, jnp.max(product, axis=0))

    peak1[0] = lax.fori_loop(0, rows // top_rows, peak_step, high)

    def peak_copy(ref, k, to, phase):
        return pltpu.make_async_remote_copy(
            src_ref=ref.at[0],
            dst_ref=ref.at[k],
            send_sem=peak_send.at[phase],
            recv_sem=peak_recv.at[phase],
            device_id=to,
            device_id_type=MESH,
        )

    more = 2 * has_low.astype(jnp.int32) + 2 * has_high.astype(jnp.int32)
    pl.semaphore_wait(barrier, inner + outer - 2 + more)

    for k in range(1, inner):
        peak_copy(peak1, k, inner_id(k), 0).start()
    @pl.when(has_high)
    def _():
        for name in "xtvme":
            for copy in halo_copies(name, True):
                copy.start()

    @pl.when(has_low)
    def _():
        for name in "xtvme":
            for copy in halo_copies(name, False):
                copy.start()

    first_force(chunks[1])
    wait("v")
    first_force(chunks[2])
    mix_rows(*chunks[0])
    mix_rows(*chunks[1])
    wait_halo("x", "t", "v")
    pack(-1, edge)
    pack(pairs - edge + 1, edge)
    first_force(*edges)
    mix_rows(*chunks[2])
    for first, n in edges:
        mix_rows(first, n)

    arrived1 = peak1.at[pl.ds(1, inner - 1)]
    pltpu.make_async_copy(arrived1, arrived1, peak_recv.at[0]).wait()
    peak2[0] = jnp.max(peak1[...], axis=0)
    for k in range(1, outer):
        peak_copy(peak2, k, outer_id(k), 1).start()

    pick_row = iota((COMPS * CODES, LANES), 0)
    pick_lane = iota((COMPS * CODES, LANES), 1)
    comp_of = pick_row // CODES
    code_of = pick_row % CODES
    picked = (pick_lane == comp_of * EDGE + code_of % EDGE) & (pick_lane < COMPS * EDGE)
    found_table = jnp.zeros((COMPS * CODES, LOW), F32)
    for h in range(blocks):
        pick = jnp.where(picked & (code_of // EDGE == h), 1.0, 0.0).astype(BF16)
        found_table += dot_t(pick, mixm[pl.ds(h * LOW, LOW), :])
    table[...] = found_table.astype(BF16)

    def trace_copy(j):
        return pltpu.make_async_remote_copy(
            src_ref=sent.at[j],
            dst_ref=got.at[2 - j],
            send_sem=trace_send.at[j],
            recv_sem=trace_recv.at[2 - j],
            device_id={"grp": 1 - g, "patch": p + (j - 1)},
            device_id_type=MESH,
        )

    def guarded(cond, run):
        if cond is None:
            run()
        else:
            pl.when(cond)(run)

    code_id = iota((CODES, third), 0)

    for j in (0, 2, 1):
        result = jnp.zeros((SEG, third), F32)
        for q in range(3):
            found = dot(table[...], hot[j, :, parts[q]])
            mask = code_id == code_ref[pl.ds(j, 1), parts[q]]
            for c in range(COMPS):
                chosen = jnp.where(mask, found[c * CODES : (c + 1) * CODES], 0.0)
                result = jnp.where(
                    row16 == c * 3 + q, jnp.sum(chosen, axis=0, keepdims=True), result
                )
        own[j] = result
        sent[j] = result.astype(BF16)
        guarded(exists[j], lambda j=j: trace_copy(j).start())

    wait("e")
    wait_halo("m", "e")

    def prepare(i, carry):
        for k in range(10):
            j = i * 10 + k
            at = (i * 5 + k // 2, k % 2)
            mass = rows_of(ms, seg_len, j)
            coef = mass * rows_of(ts, seg_len, j)
            applied = three(mass) * wide_rows_of(es, seg_len, j)
            ao[at] = applied
            co[at] = coef
            dd[at] = mass
            sbuf[at] = applied - three(coef) * sbuf[at]
            wo[at] = wide_rows_of(vs, seg_len, j)
            xo[at] = wide_rows_of(xs, seg_len, j)
        return carry

    lax.fori_loop(0, seg_len // 10, prepare, 0)

    for j in range(3):
        guarded(exists[j], lambda j=j: trace_copy(2 - j).wait_recv())
    zero = jnp.zeros((CODES, third), BF16)
    sums = []
    for j in range(3):
        value = (got[j].astype(F32) - own[j]) * wl[j]
        coarse = value.astype(BF16).astype(F32)
        fine = value - coarse
        for q in range(3):
            mask = code_id == code_ref[pl.ds(j, 1), parts[q]]
            stack = []
            for piece in (coarse, fine):
                for c in range(COMPS):
                    one = piece[c * 3 + q : c * 3 + q + 1]
                    stack.append(jnp.where(mask, one, 0.0).astype(BF16))
                stack.append(zero)
            sums.append(dot_t(hot[j, :, parts[q]], jnp.concatenate(stack, axis=0)))
    summed = sum(sums[0::2]) + sum(sums[1::2])
    both = summed[:, :LANES] + summed[:, LANES:]
    acc[...] = both
    first = both.astype(BF16)
    pieces = jnp.concatenate([first, (both - first.astype(F32)).astype(BF16)], axis=1)

    fine_group = g == 1

    def edge_lane_rows(first_row):
        out = []
        for k in range(HALO):
            j = (first_row + k + BASE) % seg_len
            s = (first_row + k + BASE) // seg_len
            one = acc[pl.ds((j % SEG) * SEG + s, 1), :]
            keep = iota((1, LANES), 1) % CODES // EDGE == j // SEG
            out.append(jnp.where(keep, one, 0.0))
        return jnp.concatenate(out, axis=0)

    far_src[0] = edge_lane_rows(0)
    far_src[1] = edge_lane_rows(rows - HALO)

    def far_copy(up):
        return pltpu.make_async_remote_copy(
            src_ref=far_src.at[int(up)],
            dst_ref=far_dst.at[1 - int(up)],
            send_sem=far_send.at[int(up)],
            recv_sem=far_recv.at[int(up)],
            device_id={"grp": g, "patch": p + 1 if up else p - 1},
            device_id_type=MESH,
        )

    pl.when(jnp.logical_not(fine_group & has_low))(
        lambda: far_dst.at[0].__setitem__(..., jnp.zeros((HALO, LANES), F32))
    )
    pl.when(jnp.logical_not(fine_group & has_high))(
        lambda: far_dst.at[1].__setitem__(..., jnp.zeros((HALO, LANES), F32))
    )
    pl.when(fine_group & has_high)(lambda: far_copy(True).start())
    pl.when(fine_group & has_low)(lambda: far_copy(False).start())

    arrived2 = peak2.at[pl.ds(1, outer - 1)]
    pltpu.make_async_copy(arrived2, arrived2, peak_recv.at[1]).wait()
    top = jnp.max(jnp.max(peak2[...], axis=0), axis=(0, 1), keepdims=True)
    base_step = COURANT * (1.0 / jnp.sqrt(top))
    size = jnp.where(g == 0, SUBSTEPS * base_step, base_step)
    square = size * size
    half = SEG // 2

    def finish(h):
        n = min(half, pairs - h * half)
        placed = dot(pieces[: 2 * n * SEG], place[h]).reshape(n, 2, SEG, width)
        for k in range(n):
            for par in range(2):
                at = (h * half + k, par)
                extra = three(dd[at]) * placed[k, par]
                moved = size * wo[at] + square * (sbuf[at] + extra)
                there = xo[at] + moved
                ao[at] = square * (ao[at] + extra)
                co[at] = square * co[at]
                wo[at] = moved
                xo[at] = there
                xb1[at[0] + 1, par] = there.astype(BF16)

    @pl.when(g == 0)
    def _():
        for h in range(blocks):
            finish(h)

    @pl.when(fine_group)
    def _():
        done = 0
        for first, n in chunks:
            ready = blocks if first + n == chunks[-1][0] + chunks[-1][1] else (first + n) // half + 1
            for h in range(done, ready):
                finish(h)
            done = ready
            advance(pair_force(xb1, band, band_mid, (first, n)), (xo, wo), (xo, wo), ao, co, xb2, (first, n))

    pl.when(fine_group & has_low)(lambda: far_copy(True).wait_recv())
    pl.when(fine_group & has_high)(lambda: far_copy(False).wait_recv())
    any_place = place[0]
    for h in range(1, blocks):
        any_place = any_place + place[h]
    far = far_dst[...].reshape(2 * HALO, LANES)
    far_first = far.astype(BF16)
    far_pieces = jnp.concatenate([far_first, (far - far_first.astype(F32)).astype(BF16)], axis=1)
    far_placed = dot(far_pieces, any_place)
    seg_id = iota((SEG, width), 0)
    for side, first_row in ((0, -HALO), (1, rows)):
        for k in range(HALO):
            j = (first_row + k + BASE) % seg_len
            s = (first_row + k + BASE) // seg_len
            at = (j // 2, j % 2)
            one = far_placed[side * HALO + k : side * HALO + k + 1]
            extra = square * three(dd[at]) * jnp.where(seg_id == s, one, 0.0)
            there = xo[at] + extra
            ao[at] = ao[at] + extra
            wo[at] = wo[at] + extra
            xo[at] = there
            xb1[at[0] + 1, at[1]] = there.astype(BF16)
    for par in range(2):
        xb1[0, par] = pltpu.roll(xo[pairs - 1, par], 1, 0).astype(BF16)
        xb1[pairs + 1, par] = pltpu.roll(xo[0, par], SEG - 1, 0).astype(BF16)
    size_out[...] = jnp.broadcast_to(1.0 / size, size_out.shape)

    @pl.when(has_high)
    def _():
        for name in "xtvme":
            for copy in halo_copies(name, True):
                copy.wait_send()

    @pl.when(has_low)
    def _():
        for name in "xtvme":
            for copy in halo_copies(name, False):
                copy.wait_send()

    for j in range(3):
        guarded(exists[j], lambda j=j: trace_copy(j).wait_send())
    pl.when(fine_group & has_high)(lambda: far_copy(True).wait_send())
    pl.when(fine_group & has_low)(lambda: far_copy(False).wait_send())
    pltpu.make_async_copy(arrived1, arrived1, peak_send.at[0]).wait()
    pltpu.make_async_copy(arrived2, arrived2, peak_send.at[1]).wait()


def steps_kernel(
    x1, w1, a, c, xb1, mids, band, band_mid, inverse, disp_out, vel_out, xo, wo, xb2, xb3, xs, vs, out_sem
):
    g = lax.axis_index("grp")
    rows = disp_out.shape[1]
    width = disp_out.shape[2]
    total = rows + 2 * BASE
    seg_len = total // SEG
    pairs = seg_len // 2
    scale = inverse[0:1, 0:1]

    def put(i, par, x, w):
        j = 2 * i + par
        v = w * scale
        for value, ref in ((x, xs), (v, vs)):
            for c in range(COMPS):
                for half in range(2):
                    at = pl.ds(OFF + j + half * 8 * seg_len, 8, stride=seg_len)
                    ref[c, at, :] = value[half * 8 : half * 8 + 8, c * LANES : (c + 1) * LANES]

    def drain():
        copies = []
        for k, (ref, out) in enumerate(((xs, disp_out), (vs, vel_out))):
            for c in range(COMPS):
                copies.append(
                    pltpu.make_async_copy(
                        ref.at[c, pl.ds(OFF + BASE, rows)],
                        out.at[0, :, pl.ds(c * LANES, LANES)],
                        out_sem.at[k, c],
                    )
                )
        for copy in copies:
            copy.start()
        for copy in copies:
            copy.wait()

    @pl.when(g == 0)
    def _():
        def move(i, carry):
            for par in range(2):
                put(i, par, x1[i, par], w1[i, par])
            return carry

        lax.fori_loop(0, pairs, move, 0)
        drain()

    @pl.when(g == 1)
    def _():
        _, chunks, edges = row_ranges(pairs)
        order = [[chunks[1]], [chunks[0]], [chunks[2]], edges]
        middle = pl.ds(chunks[0][0] + 1, sum(n for _, n in chunks))

        def wrap(nxt):
            for par in range(2):
                nxt[0, par] = pltpu.roll(xo[pairs - 1, par], 1, 0).astype(BF16)
                nxt[pairs + 1, par] = pltpu.roll(xo[0, par], SEG - 1, 0).astype(BF16)

        sums = pair_force(xb1, band, band_mid, *edges)
        advance(sums, (x1, w1), (xo, wo), a, c, xb2, *edges)
        xb2[middle] = mids[middle]
        wrap(xb2)
        for ranges in order:
            src = (xo, wo) if ranges is edges else (x1, w1)
            sums = pair_force(xb2, band, band_mid, *ranges)
            advance(sums, src, (xo, wo), a, c, xb3, *ranges)
        wrap(xb3)
        for ranges in order:
            sums = pair_force(xb3, band, band_mid, *ranges)
            done = 0
            for first, n in ranges:
                for i in range(n):
                    for par in range(2):
                        at = (first + i, par)
                        w = wo[at] + a[at] - three(c[at]) * sums[par][done + i]
                        put(first + i, par, xo[at] + w, w)
                done += n
        drain()


def per_device(
    n_grp,
    n_patch,
    displace,
    velocity,
    ext_force,
    inv_mass,
    thickness,
    stiff_bands,
    pair_points,
    pair_weights,
):
    rows, width = displace.shape[1:]
    slots = pair_points.shape[3]
    total = rows + 2 * BASE
    seg_len = total // SEG
    pairs = seg_len // 2
    blocks = -(-seg_len // SEG)
    third = slots // 3
    taps = stiff_bands.shape[0]
    bands = stiff_bands.reshape(taps * width, width)
    points = pair_points.reshape(3, 1, slots)
    weights = pair_weights.reshape(3, 1, slots)
    hbm = pl.BlockSpec(memory_space=pltpu.HBM)
    vmem = pl.BlockSpec(memory_space=pltpu.VMEM)
    dma = pltpu.SemaphoreType.DMA
    lined = total + 2 * OFF
    wide = pltpu.VMEM((COMPS, lined, LANES), F32)
    slim = pltpu.VMEM((lined, LANES), F32)
    seg_wide = pltpu.VMEM((pairs, 2, SEG, width), F32)
    seg_slim = pltpu.VMEM((pairs, 2, SEG, LANES), F32)
    seg_bf16 = pltpu.VMEM((pairs + 2, 2, SEG, width), BF16)
    state = pl.pallas_call(
        functools.partial(kernel, n_grp, n_patch),
        out_shape=[
            seg_wide,
            seg_wide,
            seg_wide,
            seg_slim,
            seg_bf16,
            seg_bf16,
            pltpu.VMEM(bands.shape, BF16),
            pltpu.VMEM(((taps + 1) * width, 2 * LANES), BF16),
            pltpu.VMEM((8, LANES), F32),
        ],
        in_specs=[hbm] * 8,
        out_specs=[vmem] * 9,
        scratch_shapes=[
            wide,
            wide,
            wide,
            slim,
            slim,
            seg_bf16,
            seg_wide,
            seg_slim,
            pltpu.VMEM((blocks * LOW, LANES), BF16),
            pltpu.VMEM((COMPS * CODES, LOW), BF16),
            pltpu.VMEM((3, LOW, slots), BF16),
            pltpu.VMEM((blocks, LOW, width), BF16),
            pltpu.VMEM((3, 1, slots), jnp.int32),
            pltpu.VMEM((3, slots), jnp.int32),
            pltpu.VMEM((3, 1, slots), F32),
            pltpu.VMEM((3, slots), jnp.int32),
            pltpu.VMEM((3, SEG, third), F32),
            pltpu.VMEM((3, SEG, third), F32),
            pltpu.VMEM((3, SEG, third), BF16),
            pltpu.VMEM((3, SEG, third), BF16),
            pltpu.VMEM((LOW, LANES), F32),
            pltpu.VMEM((2, HALO, LANES), F32),
            pltpu.VMEM((2, HALO, LANES), F32),
            pltpu.VMEM((n_grp * INNER, 8, LANES), F32),
            pltpu.VMEM((n_patch // INNER, 8, LANES), F32),
            dma((16,)),
            dma((11, 2)),
            dma((11, 2)),
            dma((3,)),
            dma((3,)),
            dma((2,)),
            dma((2,)),
            dma((2,)),
            dma((2,)),
        ],
        compiler_params=pltpu.CompilerParams(
            has_side_effects=True, collective_id=0, vmem_limit_bytes=44 * 1024 * 1024
        ),
        name="couple_step",
    )(displace, velocity, ext_force, inv_mass, thickness, bands, points, weights)
    return pl.pallas_call(
        steps_kernel,
        out_shape=[jax.ShapeDtypeStruct(displace.shape, F32)] * 2,
        in_specs=[vmem] * 9,
        out_specs=[hbm] * 2,
        scratch_shapes=[seg_wide, seg_wide, seg_bf16, seg_bf16, wide, wide, dma((2, COMPS))],
        compiler_params=pltpu.CompilerParams(vmem_limit_bytes=20 * 1024 * 1024),
        name="fine_steps",
    )(*state)


def solution(mesh):
    return jax.shard_map(
        functools.partial(per_device, mesh.shape["grp"], mesh.shape["patch"]),
        mesh=mesh,
        in_specs=(
            P("grp", "patch", None),
            P("grp", "patch", None),
            P("grp", "patch", None),
            P("grp", "patch", None),
            P("grp", "patch", None),
            P(),
            P("grp", "patch", None, None),
            P("grp", "patch", None, None),
        ),
        out_specs=(P("grp", "patch", None), P("grp", "patch", None)),
        check_vma=False,
    )
```

```python
import functools

import jax
import jax.numpy as jnp
from jax import lax
from jax.experimental import pallas as pl
from jax.experimental.pallas import tpu as pltpu
from jax.sharding import PartitionSpec as P

POINTS = 128
REACH = 2
SUBSTEPS = 4
EDGE = 3
COURANT = 0.4
HALO = REACH * SUBSTEPS
BASE = 2 * HALO
LANES = 128
COMPS = 3
SEG = 16
OFF = 8
INNER = 4
CODES = 32
LOW = 256
F32 = jnp.float32
BF16 = jnp.bfloat16
MESH = pl.DeviceIdType.MESH


def iota(shape, dim):
    return lax.broadcasted_iota(jnp.int32, shape, dim)


def dot(a, b):
    return jnp.dot(a, b, preferred_element_type=F32)


def dot_t(a, b):
    return lax.dot_general(a, b, (((1,), (1,)), ((), ())), preferred_element_type=F32)


def apart(index, a):
    return jnp.where(index >= 0, a, 0.0)


def split_even(total, parts):
    base, extra = divmod(total, parts)
    sizes = [base + (i < extra) for i in range(parts)]
    return [(sum(sizes[:i]), n) for i, n in enumerate(sizes)]


def pair_force(xb, band, band_mid, *ranges):
    width = xb.shape[3]
    taps = []
    for r in range(2 * REACH + 2):
        got = [
            xb[pl.ds(first + (r - REACH) // 2 + 1, n), r % 2].reshape(n * SEG, width)
            for first, n in ranges
        ]
        taps.append(got[0] if len(got) == 1 else jnp.concatenate(got, axis=0))
    n = sum(n for _, n in ranges)
    lhs = jnp.concatenate(taps, axis=1)
    span = (2 * REACH + 1) * width
    low = dot(lhs[:, :span], band[:, : 2 * LANES])
    mid = dot(lhs, band_mid[...])
    high = dot(lhs[:, width:], band[:, LANES:])
    even = jnp.concatenate([low, mid[:, :LANES]], axis=1)
    odd = jnp.concatenate([mid[:, LANES:], high], axis=1)
    return even.reshape(n, SEG, width), odd.reshape(n, SEG, width)


def advance(sums, src, dst, a, c, nxt, *ranges):
    done = 0
    for first, n in ranges:
        here = pl.ds(first, n)
        for par in range(2):
            inner = sums[par][done : done + n]
            w = src[1][here, par] + a[here, par] - three(c[here, par]) * inner
            x = src[0][here, par] + w
            dst[0][here, par] = x
            dst[1][here, par] = w
            nxt[pl.ds(first + 1, n), par] = x.astype(BF16)
        done += n


def row_ranges(pairs):
    edge = (BASE + REACH) // 2
    chunks = [(edge + first, n) for first, n in split_even(pairs - 2 * edge, 3)]
    return edge, chunks, [(0, edge), (pairs - edge, edge)]


def rows_of(ref, seg_len, j):
    return jnp.concatenate(
        [ref[pl.ds(OFF + j + half * 8 * seg_len, 8, stride=seg_len), :] for half in range(2)], axis=0
    )


def wide_rows_of(ref, seg_len, j):
    return jnp.concatenate([rows_of(ref.at[c], seg_len, j) for c in range(COMPS)], axis=1)


def three(a):
    return jnp.concatenate([a, a, a], axis=-1)


def kernel(
    n_grp,
    n_patch,
    disp_hbm,
    vel_hbm,
    ext_hbm,
    mass_hbm,
    thick_hbm,
    band_hbm,
    pts_hbm,
    wts_hbm,
    xo,
    wo,
    ao,
    co,
    xb1,
    xb2,
    band,
    band_mid,
    size_out,
    xs,
    vs,
    es,
    ms,
    ts,
    xb0,
    sbuf,
    dd,
    mixm,
    table,
    hot,
    place,
    pts_in,
    pts,
    wts,
    code_ref,
    wl,
    own,
    sent,
    got,
    acc,
    far_src,
    far_dst,
    peak1,
    peak2,
    load_sem,
    halo_send,
    halo_recv,
    trace_send,
    trace_recv,
    far_send,
    far_recv,
    peak_send,
    peak_recv,
):
    g = lax.axis_index("grp")
    p = lax.axis_index("patch")
    rows = disp_hbm.shape[1]
    width = disp_hbm.shape[2]
    slots = pts_hbm.shape[2]
    total = rows + 2 * BASE
    seg_len = total // SEG
    pairs = seg_len // 2
    blocks = -(-seg_len // SEG)
    start = OFF + BASE
    own_rows = pl.ds(start, rows)
    has_low = p > 0
    has_high = p < n_patch - 1
    lanes = [pl.ds(c * LANES, LANES) for c in range(COMPS)]
    span = (2 * REACH + 1) * width

    def load(src, dst, k):
        return pltpu.make_async_copy(src, dst, load_sem.at[k])

    loads = {
        "pts": [load(pts_hbm, pts_in, 0), load(wts_hbm, wts, 1)],
        "x": [load(disp_hbm.at[0, :, lanes[c]], xs.at[c, own_rows], 2 + c) for c in range(COMPS)],
        "band": [load(band_hbm, band, 5)],
        "t": [load(thick_hbm.at[0], ts.at[own_rows], 8)],
        "m": [load(mass_hbm.at[0], ms.at[own_rows], 12)],
        "v": [load(vel_hbm.at[0, :, lanes[c]], vs.at[c, own_rows], 9 + c) for c in range(COMPS)],
        "e": [load(ext_hbm.at[0, :, lanes[c]], es.at[c, own_rows], 13 + c) for c in range(COMPS)],
    }

    def begin(*names):
        for name in names:
            for copy in loads[name]:
                copy.start()

    begin("pts", "band", "x")

    def wait(*names):
        for name in names:
            for copy in loads[name]:
                copy.wait()

    inner = n_grp * INNER
    outer = n_patch // INNER
    mine_in = g * INNER + p % INNER
    mine_out = p // INNER

    def inner_id(k):
        to = (mine_in + k) % inner
        return {"grp": to // INNER, "patch": mine_out * INNER + to % INNER}

    def outer_id(k):
        return {"grp": g, "patch": (mine_out + k) % outer * INNER + p % INNER}

    barrier = pltpu.get_barrier_semaphore()

    def greet(device_id):
        pl.semaphore_signal(barrier, inc=1, device_id=device_id, device_id_type=MESH)

    for k in range(1, inner):
        greet(inner_id(k))
    for k in range(1, outer):
        greet(outer_id(k))

    @pl.when(has_low)
    def _():
        for to in (g, 1 - g):
            greet({"grp": to, "patch": p - 1})

    @pl.when(has_high)
    def _():
        for to in (g, 1 - g):
            greet({"grp": to, "patch": p + 1})

    def zero_rows(at, n):
        for ref in (xs, vs, es):
            for c in range(COMPS):
                ref[c, pl.ds(at, n), :] = jnp.zeros((n, LANES), F32)
        for ref in (ms, ts):
            ref[pl.ds(at, n), :] = jnp.zeros((n, LANES), F32)

    zero_rows(0, start - HALO)
    zero_rows(start + rows + HALO, start - HALO)
    pl.when(p == 0)(lambda: zero_rows(start - HALO, HALO))
    pl.when(p == n_patch - 1)(lambda: zero_rows(start + rows, HALO))
    band_mid[pl.ds(span, width), lanes[0]] = jnp.zeros((width, LANES), BF16)
    band_mid[pl.ds(0, width), lanes[1]] = jnp.zeros((width, LANES), BF16)
    for c in range(seg_len * SEG, blocks * LOW, SEG):
        mixm[pl.ds(c, SEG), :] = jnp.zeros((SEG, LANES), BF16)

    wait("pts")
    entry = pts_in[...].reshape(3, slots)
    row = entry // EDGE
    point = entry - row * EDGE
    row = row + BASE
    seg = row // seg_len
    j_row = row - seg * seg_len
    block = j_row // SEG
    code_ref[...] = block * EDGE + point
    pts[...] = (j_row - block * SEG) * SEG + seg
    third = slots // 3
    parts = [pl.ds(q * third, third) for q in range(3)]
    low_id = iota((LOW, third), 0)
    row16 = iota((SEG, third), 0)
    exists = (has_low, None, has_high)
    for j in range(3):
        weight = jnp.zeros((SEG, third), F32)
        for q in range(3):
            low = pts[pl.ds(j, 1), parts[q]]
            hot[j, :, parts[q]] = jnp.where(low_id == low, 1.0, 0.0).astype(BF16)
            weight = jnp.where(row16 % 3 == q, wts[j, :, parts[q]], weight)
        present = 1.0 if exists[j] is None else jnp.where(exists[j], 1.0, 0.0)
        wl[j] = jnp.where(row16 < 3 * COMPS, weight * present, 0.0)

    begin("t", "m", "v", "e")
    place_row = iota((LOW, width), 0) % LANES
    place_lane = iota((LOW, width), 1)
    comp_row = place_row // CODES
    code_row = place_row % CODES
    hit = (comp_row == place_lane // POINTS) & (code_row % EDGE == place_lane % POINTS)
    for h in range(blocks):
        place[h] = jnp.where(hit & (code_row // EDGE == h), 1.0, 0.0).astype(BF16)

    @pl.when(p == 0)
    def _():
        got[0] = jnp.zeros(got.shape[1:], BF16)

    @pl.when(p == n_patch - 1)
    def _():
        got[2] = jnp.zeros(got.shape[1:], BF16)

    def halo_copies(name, up):
        src = pl.ds(start + rows - HALO if up else start, HALO)
        dst = pl.ds(start - HALO if up else start + rows, HALO)
        to = p + 1 if up else p - 1
        target, k = {"x": (xs, 0), "v": (vs, 3), "e": (es, 6), "m": (ms, 9), "t": (ts, 10)}[name]
        if name in "xve":
            refs = [(target.at[c, src], target.at[c, dst]) for c in range(COMPS)]
        else:
            refs = [(target.at[src], target.at[dst])]
        return [
            pltpu.make_async_remote_copy(
                src_ref=a,
                dst_ref=b,
                send_sem=halo_send.at[k + i, int(up)],
                recv_sem=halo_recv.at[k + i, int(up)],
                device_id={"grp": g, "patch": to},
                device_id_type=MESH,
            )
            for i, (a, b) in enumerate(refs)
        ]

    def start_halo(*names):
        @pl.when(has_high)
        def _():
            for name in names:
                for copy in halo_copies(name, True):
                    copy.start()

        @pl.when(has_low)
        def _():
            for name in names:
                for copy in halo_copies(name, False):
                    copy.start()

    def wait_halo(*names):
        @pl.when(has_low)
        def _():
            for name in names:
                for copy in halo_copies(name, True):
                    copy.wait_recv()

        @pl.when(has_high)
        def _():
            for name in names:
                for copy in halo_copies(name, False):
                    copy.wait_recv()

    def pack(first, n):
        for i in range(first, first + n):
            for par in range(2):
                xb0[i + 1, par] = wide_rows_of(xs, seg_len, 2 * i + par).astype(BF16)

    lane = iota((SEG, LANES), 1)

    def mix_rows(first, n):
        for i in range(first, first + n):
            for par in range(2):
                j = 2 * i + par
                thick = rows_of(ts, seg_len, j)
                mixed = []
                for c in range(COMPS):
                    f = thick * sbuf[i, par, :, lanes[c]]
                    mixed.append(
                        rows_of(xs.at[c], seg_len, j) + 0.5 * (rows_of(vs.at[c], seg_len, j) + f)
                    )
                out = jnp.where(lane < 3, mixed[0], 0.0)
                out = jnp.where((lane >= 3) & (lane < 6), pltpu.roll(mixed[1], 3, 1), out)
                out = jnp.where((lane >= 6) & (lane < 9), pltpu.roll(mixed[2], 6, 1), out)
                mixm[pl.ds(j * SEG, SEG), :] = out.astype(BF16)

    def first_force(*ranges):
        done = 0
        sums = pair_force(xb0, band, band_mid, *ranges)
        for first, n in ranges:
            for par in range(2):
                sbuf[pl.ds(first, n), par] = sums[par][done : done + n]
            done += n

    edge, chunks, edges = row_ranges(pairs)
    wait("band")
    band_mid[pl.ds(0, span), lanes[0]] = band[:, lanes[2]]
    band_mid[pl.ds(width, span), lanes[1]] = band[:, lanes[0]]
    wait("x")
    pack(edge - 1, pairs - 2 * edge + 2)
    first_force(chunks[0])
    wait("t", "m")
    top_rows = 256
    high = jnp.zeros((8, LANES), F32)

    def peak_step(i, high):
        at = pl.ds(pl.multiple_of(start + i * top_rows, 8), top_rows)
        product = (ms[at, :] * ts[at, :]).reshape(top_rows // 8, 8, LANES)
        return jnp.maximum(high, jnp.max(product, axis=0))

    peak1[0] = lax.fori_loop(0, rows // top_rows, peak_step, high)

    def peak_copy(ref, k, to, phase):
        return pltpu.make_async_remote_copy(
            src_ref=ref.at[0],
            dst_ref=ref.at[k],
            send_sem=peak_send.at[phase],
            recv_sem=peak_recv.at[phase],
            device_id=to,
            device_id_type=MESH,
        )

    more = 2 * has_low.astype(jnp.int32) + 2 * has_high.astype(jnp.int32)
    pl.semaphore_wait(barrier, inner + outer - 2 + more)

    for k in range(1, inner):
        peak_copy(peak1, k, inner_id(k), 0).start()
    start_halo("x", "t", "m")
    first_force(chunks[1])
    wait("v", "e")
    start_halo("v", "e")
    first_force(chunks[2])
    mix_rows(*chunks[0])
    mix_rows(*chunks[1])
    wait_halo("x")
    pack(-1, edge)
    pack(pairs - edge + 1, edge)
    first_force(*edges)
    mix_rows(*chunks[2])
    wait_halo("t", "v")
    for first, n in edges:
        mix_rows(first, n)

    arrived1 = peak1.at[pl.ds(1, inner - 1)]
    pltpu.make_async_copy(arrived1, arrived1, peak_recv.at[0]).wait()
    peak2[0] = jnp.max(peak1[...], axis=0)
    for k in range(1, outer):
        peak_copy(peak2, k, outer_id(k), 1).start()

    pick_row = iota((COMPS * CODES, LANES), 0)
    pick_lane = iota((COMPS * CODES, LANES), 1)
    comp_of = pick_row // CODES
    code_of = pick_row % CODES
    picked = (pick_lane == comp_of * EDGE + code_of % EDGE) & (pick_lane < COMPS * EDGE)
    found = []
    for h in range(blocks):
        pick = jnp.where(picked & (code_of // EDGE == h), 1.0, 0.0).astype(BF16)
        found.append(dot_t(pick, mixm[pl.ds(h * LOW, LOW), :]))
    table[...] = (apart(p, sum(found[0::2])) + sum(found[1::2])).astype(BF16)

    def trace_copy(j):
        return pltpu.make_async_remote_copy(
            src_ref=sent.at[j],
            dst_ref=got.at[2 - j],
            send_sem=trace_send.at[j],
            recv_sem=trace_recv.at[2 - j],
            device_id={"grp": 1 - g, "patch": p + (j - 1)},
            device_id_type=MESH,
        )

    def guarded(cond, run):
        if cond is None:
            run()
        else:
            pl.when(cond)(run)

    code_id = iota((CODES, third), 0)

    for j in (0, 2, 1):
        result = jnp.zeros((SEG, third), F32)
        for q in range(3):
            found = dot(table[...], hot[j, :, parts[q]])
            mask = code_id == code_ref[pl.ds(j, 1), parts[q]]
            for c in range(COMPS):
                chosen = jnp.where(mask, found[c * CODES : (c + 1) * CODES], 0.0)
                result = jnp.where(
                    row16 == c * 3 + q, jnp.sum(chosen, axis=0, keepdims=True), result
                )
        own[j] = result
        sent[j] = result.astype(BF16)
    for j in (0, 2, 1):
        guarded(exists[j], lambda j=j: trace_copy(j).start())

    wait_halo("m", "e")

    def prepare(i, carry):
        for k in range(10):
            j = i * 10 + k
            at = (i * 5 + k // 2, k % 2)
            mass = rows_of(ms, seg_len, j)
            coef = mass * rows_of(ts, seg_len, j)
            applied = three(mass) * wide_rows_of(es, seg_len, j)
            ao[at] = applied
            co[at] = coef
            dd[at] = mass
            sbuf[at] = applied - three(coef) * sbuf[at]
            wo[at] = wide_rows_of(vs, seg_len, j)
            xo[at] = wide_rows_of(xs, seg_len, j)
        return carry

    lax.fori_loop(0, seg_len // 10, prepare, 0)

    for j in range(3):
        guarded(exists[j], lambda j=j: trace_copy(2 - j).wait_recv())
    zero = jnp.zeros((CODES, third), BF16)
    sums = []
    for j in range(3):
        value = (got[j].astype(F32) - own[j]) * wl[j]
        coarse = value.astype(BF16).astype(F32)
        fine = value - coarse
        for q in range(3):
            mask = code_id == code_ref[pl.ds(j, 1), parts[q]]
            stack = []
            for piece in (coarse, fine):
                for c in range(COMPS):
                    one = piece[c * 3 + q : c * 3 + q + 1]
                    stack.append(jnp.where(mask, one, 0.0).astype(BF16))
                stack.append(zero)
            sums.append(dot_t(hot[j, :, parts[q]], jnp.concatenate(stack, axis=0)))
    summed = apart(p, sum(sums[0::2])) + sum(sums[1::2])
    both = summed[:, :LANES] + summed[:, LANES:]
    acc[...] = both
    first = both.astype(BF16)
    pieces = jnp.concatenate([first, (both - first.astype(F32)).astype(BF16)], axis=1)

    fine_group = g == 1

    def edge_lane_rows(first_row):
        out = []
        for k in range(HALO):
            j = (first_row + k + BASE) % seg_len
            s = (first_row + k + BASE) // seg_len
            one = acc[pl.ds((j % SEG) * SEG + s, 1), :]
            keep = iota((1, LANES), 1) % CODES // EDGE == j // SEG
            out.append(jnp.where(keep, one, 0.0))
        return jnp.concatenate(out, axis=0)

    far_src[0] = edge_lane_rows(0)
    far_src[1] = edge_lane_rows(rows - HALO)

    def far_copy(up):
        return pltpu.make_async_remote_copy(
            src_ref=far_src.at[int(up)],
            dst_ref=far_dst.at[1 - int(up)],
            send_sem=far_send.at[int(up)],
            recv_sem=far_recv.at[int(up)],
            device_id={"grp": g, "patch": p + 1 if up else p - 1},
            device_id_type=MESH,
        )

    pl.when(jnp.logical_not(fine_group & has_low))(
        lambda: far_dst.at[0].__setitem__(..., jnp.zeros((HALO, LANES), F32))
    )
    pl.when(jnp.logical_not(fine_group & has_high))(
        lambda: far_dst.at[1].__setitem__(..., jnp.zeros((HALO, LANES), F32))
    )
    pl.when(fine_group & has_high)(lambda: far_copy(True).start())
    pl.when(fine_group & has_low)(lambda: far_copy(False).start())

    arrived2 = peak2.at[pl.ds(1, outer - 1)]
    pltpu.make_async_copy(arrived2, arrived2, peak_recv.at[1]).wait()
    top = jnp.max(jnp.max(peak2[...], axis=0), axis=(0, 1), keepdims=True)
    base_step = COURANT * (1.0 / jnp.sqrt(top))
    size = jnp.where(g == 0, SUBSTEPS * base_step, base_step)
    square = size * size
    half = SEG // 2

    def finish(h):
        n = min(half, pairs - h * half)
        placed = dot(pieces[: 2 * n * SEG], place[h]).reshape(n, 2, SEG, width)
        for k in range(n):
            for par in range(2):
                at = (h * half + k, par)
                extra = three(dd[at]) * placed[k, par]
                moved = size * wo[at] + square * (sbuf[at] + extra)
                there = xo[at] + moved
                ao[at] = square * (ao[at] + extra)
                co[at] = square * co[at]
                wo[at] = moved
                xo[at] = there
                xb1[at[0] + 1, par] = there.astype(BF16)

    @pl.when(g == 0)
    def _():
        for h in range(blocks):
            finish(h)

    @pl.when(fine_group)
    def _():
        def sums_of(k):
            return pair_force(xb1, band, band_mid, chunks[k])

        def step_of(k, sums):
            advance(sums, (xo, wo), (xo, wo), ao, co, xb2, chunks[k])

        bounds = [(first + n) // half + 1 for first, n in chunks]
        for h in range(1, bounds[0]):
            finish(h)
        sums = sums_of(0)
        for h in range(bounds[0], bounds[1]):
            finish(h)
        step_of(0, sums)
        sums = sums_of(1)
        for h in [*range(bounds[1], blocks), 0]:
            finish(h)
        step_of(1, sums)
        pl.when(has_low)(lambda: far_copy(True).wait_recv())
        pl.when(has_high)(lambda: far_copy(False).wait_recv())
        sums = sums_of(2)
        any_place = place[0]
        for h in range(1, blocks):
            any_place = any_place + place[h]
        far = far_dst[...].reshape(2 * HALO, LANES)
        far_first = far.astype(BF16)
        far_pieces = jnp.concatenate([far_first, (far - far_first.astype(F32)).astype(BF16)], axis=1)
        far_placed = dot(far_pieces, any_place)
        seg_id = iota((SEG, width), 0)
        for side, first_row in ((0, -HALO), (1, rows)):
            for k in range(HALO):
                j = (first_row + k + BASE) % seg_len
                s = (first_row + k + BASE) // seg_len
                at = (j // 2, j % 2)
                one = far_placed[side * HALO + k : side * HALO + k + 1]
                extra = square * three(dd[at]) * jnp.where(seg_id == s, one, 0.0)
                there = xo[at] + extra
                ao[at] = ao[at] + extra
                wo[at] = wo[at] + extra
                xo[at] = there
                xb1[at[0] + 1, at[1]] = there.astype(BF16)
        step_of(2, sums)

    for par in range(2):
        xb1[0, par] = pltpu.roll(xo[pairs - 1, par], 1, 0).astype(BF16)
        xb1[pairs + 1, par] = pltpu.roll(xo[0, par], SEG - 1, 0).astype(BF16)
    size_out[...] = jnp.broadcast_to(1.0 / size, size_out.shape)

    @pl.when(has_high)
    def _():
        for name in "xtvme":
            for copy in halo_copies(name, True):
                copy.wait_send()

    @pl.when(has_low)
    def _():
        for name in "xtvme":
            for copy in halo_copies(name, False):
                copy.wait_send()

    for j in range(3):
        guarded(exists[j], lambda j=j: trace_copy(j).wait_send())
    pl.when(fine_group & has_high)(lambda: far_copy(True).wait_send())
    pl.when(fine_group & has_low)(lambda: far_copy(False).wait_send())
    pltpu.make_async_copy(arrived1, arrived1, peak_send.at[0]).wait()
    pltpu.make_async_copy(arrived2, arrived2, peak_send.at[1]).wait()


def steps_kernel(
    x1, w1, a, c, xb1, mids, band, band_mid, inverse, disp_out, vel_out, xo, wo, xb2, xb3, xs, vs, out_sem
):
    g = lax.axis_index("grp")
    rows = disp_out.shape[1]
    width = disp_out.shape[2]
    total = rows + 2 * BASE
    seg_len = total // SEG
    pairs = seg_len // 2
    scale = inverse[0:1, 0:1]

    def put(i, par, x, w):
        j = 2 * i + par
        v = w * scale
        for value, ref in ((x, xs), (v, vs)):
            for c in range(COMPS):
                for half in range(2):
                    at = pl.ds(OFF + j + half * 8 * seg_len, 8, stride=seg_len)
                    ref[c, at, :] = value[half * 8 : half * 8 + 8, c * LANES : (c + 1) * LANES]

    def drain():
        copies = []
        for k, (ref, out) in enumerate(((xs, disp_out), (vs, vel_out))):
            for c in range(COMPS):
                copies.append(
                    pltpu.make_async_copy(
                        ref.at[c, pl.ds(OFF + BASE, rows)],
                        out.at[0, :, pl.ds(c * LANES, LANES)],
                        out_sem.at[k, c],
                    )
                )
        for copy in copies:
            copy.start()
        for copy in copies:
            copy.wait()

    @pl.when(g == 0)
    def _():
        def move(i, carry):
            for par in range(2):
                put(i, par, x1[i, par], w1[i, par])
            return carry

        lax.fori_loop(0, pairs, move, 0)
        drain()

    @pl.when(g == 1)
    def _():
        _, chunks, edges = row_ranges(pairs)
        order = [[chunks[1]], [chunks[0]], [chunks[2]], edges]
        middle = pl.ds(chunks[0][0] + 1, sum(n for _, n in chunks))

        def wrap(nxt):
            for par in range(2):
                nxt[0, par] = pltpu.roll(xo[pairs - 1, par], 1, 0).astype(BF16)
                nxt[pairs + 1, par] = pltpu.roll(xo[0, par], SEG - 1, 0).astype(BF16)

        def first_step(sums, ranges):
            advance(sums, (x1, w1), (xo, wo), a, c, xb2, *ranges)
            wrap(xb2)

        def second_step(sums, ranges):
            src = (xo, wo) if ranges is edges else (x1, w1)
            advance(sums, src, (xo, wo), a, c, xb3, *ranges)
            if ranges is edges:
                wrap(xb3)

        def third_step(sums, ranges):
            done = 0
            for first, n in ranges:
                for i in range(n):
                    for par in range(2):
                        at = (first + i, par)
                        w = wo[at] + a[at] - three(c[at]) * sums[par][done + i]
                        put(first + i, par, xo[at] + w, w)
                done += n

        tasks = [(first_step, xb1, edges)]
        tasks += [(second_step, xb2, ranges) for ranges in order]
        tasks += [(third_step, xb3, ranges) for ranges in order]
        xb2[middle] = mids[middle]
        last = None
        for task, cur, ranges in tasks:
            sums = pair_force(cur, band, band_mid, *ranges)
            if last is not None:
                last[0](*last[1:])
            last = (task, sums, ranges)
        last[0](*last[1:])
        drain()


def per_device(
    n_grp,
    n_patch,
    displace,
    velocity,
    ext_force,
    inv_mass,
    thickness,
    stiff_bands,
    pair_points,
    pair_weights,
):
    rows, width = displace.shape[1:]
    slots = pair_points.shape[3]
    total = rows + 2 * BASE
    seg_len = total // SEG
    pairs = seg_len // 2
    blocks = -(-seg_len // SEG)
    third = slots // 3
    taps = stiff_bands.shape[0]
    bands = stiff_bands.reshape(taps * width, width)
    points = pair_points.reshape(3, 1, slots)
    weights = pair_weights.reshape(3, 1, slots)
    hbm = pl.BlockSpec(memory_space=pltpu.HBM)
    vmem = pl.BlockSpec(memory_space=pltpu.VMEM)
    dma = pltpu.SemaphoreType.DMA
    lined = total + 2 * OFF
    wide = pltpu.VMEM((COMPS, lined, LANES), F32)
    slim = pltpu.VMEM((lined, LANES), F32)
    seg_wide = pltpu.VMEM((pairs, 2, SEG, width), F32)
    seg_slim = pltpu.VMEM((pairs, 2, SEG, LANES), F32)
    seg_bf16 = pltpu.VMEM((pairs + 2, 2, SEG, width), BF16)
    state = pl.pallas_call(
        functools.partial(kernel, n_grp, n_patch),
        out_shape=[
            seg_wide,
            seg_wide,
            seg_wide,
            seg_slim,
            seg_bf16,
            seg_bf16,
            pltpu.VMEM(bands.shape, BF16),
            pltpu.VMEM(((taps + 1) * width, 2 * LANES), BF16),
            pltpu.VMEM((8, LANES), F32),
        ],
        in_specs=[hbm] * 8,
        out_specs=[vmem] * 9,
        scratch_shapes=[
            wide,
            wide,
            wide,
            slim,
            slim,
            seg_bf16,
            seg_wide,
            seg_slim,
            pltpu.VMEM((blocks * LOW, LANES), BF16),
            pltpu.VMEM((COMPS * CODES, LOW), BF16),
            pltpu.VMEM((3, LOW, slots), BF16),
            pltpu.VMEM((blocks, LOW, width), BF16),
            pltpu.VMEM((3, 1, slots), jnp.int32),
            pltpu.VMEM((3, slots), jnp.int32),
            pltpu.VMEM((3, 1, slots), F32),
            pltpu.VMEM((3, slots), jnp.int32),
            pltpu.VMEM((3, SEG, third), F32),
            pltpu.VMEM((3, SEG, third), F32),
            pltpu.VMEM((3, SEG, third), BF16),
            pltpu.VMEM((3, SEG, third), BF16),
            pltpu.VMEM((LOW, LANES), F32),
            pltpu.VMEM((2, HALO, LANES), F32),
            pltpu.VMEM((2, HALO, LANES), F32),
            pltpu.VMEM((n_grp * INNER, 8, LANES), F32),
            pltpu.VMEM((n_patch // INNER, 8, LANES), F32),
            dma((16,)),
            dma((11, 2)),
            dma((11, 2)),
            dma((3,)),
            dma((3,)),
            dma((2,)),
            dma((2,)),
            dma((2,)),
            dma((2,)),
        ],
        compiler_params=pltpu.CompilerParams(
            has_side_effects=True, collective_id=0, vmem_limit_bytes=44 * 1024 * 1024
        ),
        name="couple_step",
    )(displace, velocity, ext_force, inv_mass, thickness, bands, points, weights)
    return pl.pallas_call(
        steps_kernel,
        out_shape=[jax.ShapeDtypeStruct(displace.shape, F32)] * 2,
        in_specs=[vmem] * 9,
        out_specs=[hbm] * 2,
        scratch_shapes=[seg_wide, seg_wide, seg_bf16, seg_bf16, wide, wide, dma((2, COMPS))],
        compiler_params=pltpu.CompilerParams(vmem_limit_bytes=20 * 1024 * 1024),
        name="fine_steps",
    )(*state)


def solution(mesh):
    return jax.shard_map(
        functools.partial(per_device, mesh.shape["grp"], mesh.shape["patch"]),
        mesh=mesh,
        in_specs=(
            P("grp", "patch", None),
            P("grp", "patch", None),
            P("grp", "patch", None),
            P("grp", "patch", None),
            P("grp", "patch", None),
            P(),
            P("grp", "patch", None, None),
            P("grp", "patch", None, None),
        ),
        out_specs=(P("grp", "patch", None), P("grp", "patch", None)),
        check_vma=False,
    )
```

```python
import functools

import jax
import jax.numpy as jnp
from jax import lax
from jax.experimental import pallas as pl
from jax.experimental.pallas import tpu as pltpu
from jax.sharding import PartitionSpec as P

POINTS = 128
REACH = 2
SUBSTEPS = 4
EDGE = 3
COURANT = 0.4
HALO = REACH * SUBSTEPS
BASE = 2 * HALO
LANES = 128
COMPS = 3
SEG = 16
OFF = 8
INNER = 4
CODES = 32
LOW = 256
F32 = jnp.float32
BF16 = jnp.bfloat16
MESH = pl.DeviceIdType.MESH


def iota(shape, dim):
    return lax.broadcasted_iota(jnp.int32, shape, dim)


def dot(a, b):
    return jnp.dot(a, b, preferred_element_type=F32)


def dot_t(a, b):
    return lax.dot_general(a, b, (((1,), (1,)), ((), ())), preferred_element_type=F32)


def apart(index, a):
    return jnp.where(index >= 0, a, 0.0)


def split_even(total, parts):
    base, extra = divmod(total, parts)
    sizes = [base + (i < extra) for i in range(parts)]
    return [(sum(sizes[:i]), n) for i, n in enumerate(sizes)]


def pair_force(xb, band, band_mid, *ranges):
    width = xb.shape[3]
    taps = []
    for r in range(2 * REACH + 2):
        got = [
            xb[pl.ds(first + (r - REACH) // 2 + 1, n), r % 2].reshape(n * SEG, width)
            for first, n in ranges
        ]
        taps.append(got[0] if len(got) == 1 else jnp.concatenate(got, axis=0))
    n = sum(n for _, n in ranges)
    lhs = jnp.concatenate(taps, axis=1)
    span = (2 * REACH + 1) * width
    low = dot(lhs[:, :span], band[:, : 2 * LANES])
    mid = dot(lhs, band_mid[...])
    high = dot(lhs[:, width:], band[:, LANES:])
    even = jnp.concatenate([low, mid[:, :LANES]], axis=1)
    odd = jnp.concatenate([mid[:, LANES:], high], axis=1)
    return even.reshape(n, SEG, width), odd.reshape(n, SEG, width)


def advance(sums, src, dst, a, c, nxt, *ranges):
    done = 0
    for first, n in ranges:
        here = pl.ds(first, n)
        for par in range(2):
            inner = sums[par][done : done + n]
            w = src[1][here, par] + a[here, par] - three(c[here, par]) * inner
            x = src[0][here, par] + w
            dst[0][here, par] = x
            dst[1][here, par] = w
            nxt[pl.ds(first + 1, n), par] = x.astype(BF16)
        done += n


def row_ranges(pairs):
    edge = (BASE + REACH) // 2
    chunks = [(edge + first, n) for first, n in split_even(pairs - 2 * edge, 3)]
    return edge, chunks, [(0, edge), (pairs - edge, edge)]


def rows_of(ref, seg_len, j):
    return jnp.concatenate(
        [ref[pl.ds(OFF + j + half * 8 * seg_len, 8, stride=seg_len), :] for half in range(2)], axis=0
    )


def wide_rows_of(ref, seg_len, j):
    return jnp.concatenate([rows_of(ref.at[c], seg_len, j) for c in range(COMPS)], axis=1)


def three(a):
    return jnp.concatenate([a, a, a], axis=-1)


def kernel(
    n_grp,
    n_patch,
    disp_hbm,
    vel_hbm,
    ext_hbm,
    mass_hbm,
    thick_hbm,
    band_hbm,
    pts_hbm,
    wts_hbm,
    xo,
    wo,
    ao,
    co,
    xb1,
    xb2,
    band,
    band_mid,
    size_out,
    xs,
    vs,
    es,
    ms,
    ts,
    xb0,
    sbuf,
    dd,
    mixm,
    table,
    hot,
    place,
    pts_in,
    pts,
    wts,
    code_ref,
    wl,
    own,
    sent,
    got,
    acc,
    far_src,
    far_dst,
    peak1,
    peak2,
    load_sem,
    halo_send,
    halo_recv,
    trace_send,
    trace_recv,
    far_send,
    far_recv,
    peak_send,
    peak_recv,
):
    g = lax.axis_index("grp")
    p = lax.axis_index("patch")
    rows = disp_hbm.shape[1]
    width = disp_hbm.shape[2]
    slots = pts_hbm.shape[2]
    total = rows + 2 * BASE
    seg_len = total // SEG
    pairs = seg_len // 2
    blocks = -(-seg_len // SEG)
    start = OFF + BASE
    own_rows = pl.ds(start, rows)
    has_low = p > 0
    has_high = p < n_patch - 1
    lanes = [pl.ds(c * LANES, LANES) for c in range(COMPS)]
    span = (2 * REACH + 1) * width

    def load(src, dst, k):
        return pltpu.make_async_copy(src, dst, load_sem.at[k])

    loads = {
        "pts": [load(pts_hbm, pts_in, 0), load(wts_hbm, wts, 1)],
        "x": [load(disp_hbm.at[0, :, lanes[c]], xs.at[c, own_rows], 2 + c) for c in range(COMPS)],
        "band": [load(band_hbm, band, 5)],
        "t": [load(thick_hbm.at[0], ts.at[own_rows], 8)],
        "m": [load(mass_hbm.at[0], ms.at[own_rows], 12)],
        "v": [load(vel_hbm.at[0, :, lanes[c]], vs.at[c, own_rows], 9 + c) for c in range(COMPS)],
        "e": [load(ext_hbm.at[0, :, lanes[c]], es.at[c, own_rows], 13 + c) for c in range(COMPS)],
    }

    def begin(*names):
        for name in names:
            for copy in loads[name]:
                copy.start()

    begin("pts", "band", "x")

    def wait(*names):
        for name in names:
            for copy in loads[name]:
                copy.wait()

    inner = n_grp * INNER
    outer = n_patch // INNER
    mine_in = g * INNER + p % INNER
    mine_out = p // INNER

    def inner_id(k):
        to = (mine_in + k) % inner
        return {"grp": to // INNER, "patch": mine_out * INNER + to % INNER}

    def outer_id(k):
        return {"grp": g, "patch": (mine_out + k) % outer * INNER + p % INNER}

    barrier = pltpu.get_barrier_semaphore()

    def greet(device_id):
        pl.semaphore_signal(barrier, inc=1, device_id=device_id, device_id_type=MESH)

    for k in range(1, inner):
        greet(inner_id(k))
    for k in range(1, outer):
        greet(outer_id(k))

    @pl.when(has_low)
    def _():
        for to in (g, 1 - g):
            greet({"grp": to, "patch": p - 1})

    @pl.when(has_high)
    def _():
        for to in (g, 1 - g):
            greet({"grp": to, "patch": p + 1})

    def zero_rows(at, n):
        for ref in (xs, vs, es):
            for c in range(COMPS):
                ref[c, pl.ds(at, n), :] = jnp.zeros((n, LANES), F32)
        for ref in (ms, ts):
            ref[pl.ds(at, n), :] = jnp.zeros((n, LANES), F32)

    zero_rows(0, start - HALO)
    zero_rows(start + rows + HALO, start - HALO)
    pl.when(p == 0)(lambda: zero_rows(start - HALO, HALO))
    pl.when(p == n_patch - 1)(lambda: zero_rows(start + rows, HALO))
    band_mid[pl.ds(span, width), lanes[0]] = jnp.zeros((width, LANES), BF16)
    band_mid[pl.ds(0, width), lanes[1]] = jnp.zeros((width, LANES), BF16)
    for c in range(seg_len * SEG, blocks * LOW, SEG):
        mixm[pl.ds(c, SEG), :] = jnp.zeros((SEG, LANES), BF16)

    wait("pts")
    entry = pts_in[...].reshape(3, slots)
    row = entry // EDGE
    point = entry - row * EDGE
    row = row + BASE
    seg = row // seg_len
    j_row = row - seg * seg_len
    block = j_row // SEG
    code_ref[...] = block * EDGE + point
    pts[...] = (j_row - block * SEG) * SEG + seg
    third = slots // 3
    parts = [pl.ds(q * third, third) for q in range(3)]
    low_id = iota((LOW, third), 0)
    row16 = iota((SEG, third), 0)
    exists = (has_low, None, has_high)
    for j in range(3):
        weight = jnp.zeros((SEG, third), F32)
        for q in range(3):
            low = pts[pl.ds(j, 1), parts[q]]
            hot[j, :, parts[q]] = jnp.where(low_id == low, 1.0, 0.0).astype(BF16)
            weight = jnp.where(row16 % 3 == q, wts[j, :, parts[q]], weight)
        present = 1.0 if exists[j] is None else jnp.where(exists[j], 1.0, 0.0)
        wl[j] = jnp.where(row16 < 3 * COMPS, weight * present, 0.0)

    begin("t", "m", "v", "e")
    place_row = iota((LOW, width), 0) % LANES
    place_lane = iota((LOW, width), 1)
    comp_row = place_row // CODES
    code_row = place_row % CODES
    hit = (comp_row == place_lane // POINTS) & (code_row % EDGE == place_lane % POINTS)
    for h in range(blocks):
        place[h] = jnp.where(hit & (code_row // EDGE == h), 1.0, 0.0).astype(BF16)

    @pl.when(p == 0)
    def _():
        got[0] = jnp.zeros(got.shape[1:], BF16)

    @pl.when(p == n_patch - 1)
    def _():
        got[2] = jnp.zeros(got.shape[1:], BF16)

    def halo_copies(name, up):
        src = pl.ds(start + rows - HALO if up else start, HALO)
        dst = pl.ds(start - HALO if up else start + rows, HALO)
        to = p + 1 if up else p - 1
        target, k = {"x": (xs, 0), "v": (vs, 3), "e": (es, 6), "m": (ms, 9), "t": (ts, 10)}[name]
        if name in "xve":
            refs = [(target.at[c, src], target.at[c, dst]) for c in range(COMPS)]
        else:
            refs = [(target.at[src], target.at[dst])]
        return [
            pltpu.make_async_remote_copy(
                src_ref=a,
                dst_ref=b,
                send_sem=halo_send.at[k + i, int(up)],
                recv_sem=halo_recv.at[k + i, int(up)],
                device_id={"grp": g, "patch": to},
                device_id_type=MESH,
            )
            for i, (a, b) in enumerate(refs)
        ]

    def start_halo(*names):
        @pl.when(has_high)
        def _():
            for name in names:
                for copy in halo_copies(name, True):
                    copy.start()

        @pl.when(has_low)
        def _():
            for name in names:
                for copy in halo_copies(name, False):
                    copy.start()

    def wait_halo(*names):
        @pl.when(has_low)
        def _():
            for name in names:
                for copy in halo_copies(name, True):
                    copy.wait_recv()

        @pl.when(has_high)
        def _():
            for name in names:
                for copy in halo_copies(name, False):
                    copy.wait_recv()

    def pack(first, n):
        for i in range(first, first + n):
            for par in range(2):
                xb0[i + 1, par] = wide_rows_of(xs, seg_len, 2 * i + par).astype(BF16)

    lane = iota((SEG, LANES), 1)

    def mix_rows(first, n):
        for i in range(first, first + n):
            for par in range(2):
                j = 2 * i + par
                thick = rows_of(ts, seg_len, j)
                mixed = []
                for c in range(COMPS):
                    f = thick * sbuf[i, par, :, lanes[c]]
                    mixed.append(
                        rows_of(xs.at[c], seg_len, j) + 0.5 * (rows_of(vs.at[c], seg_len, j) + f)
                    )
                out = jnp.where(lane < 3, mixed[0], 0.0)
                out = jnp.where((lane >= 3) & (lane < 6), pltpu.roll(mixed[1], 3, 1), out)
                out = jnp.where((lane >= 6) & (lane < 9), pltpu.roll(mixed[2], 6, 1), out)
                mixm[pl.ds(j * SEG, SEG), :] = out.astype(BF16)

    def first_force(*ranges):
        done = 0
        sums = pair_force(xb0, band, band_mid, *ranges)
        for first, n in ranges:
            for par in range(2):
                sbuf[pl.ds(first, n), par] = sums[par][done : done + n]
            done += n

    edge, chunks, edges = row_ranges(pairs)
    wait("band")
    band_mid[pl.ds(0, span), lanes[0]] = band[:, lanes[2]]
    band_mid[pl.ds(width, span), lanes[1]] = band[:, lanes[0]]
    wait("x")
    pack(edge - 1, pairs - 2 * edge + 2)
    first_force(chunks[0])
    wait("t", "m")
    top_rows = 256
    high = jnp.zeros((8, LANES), F32)

    def peak_step(i, high):
        at = pl.ds(pl.multiple_of(start + i * top_rows, 8), top_rows)
        product = (ms[at, :] * ts[at, :]).reshape(top_rows // 8, 8, LANES)
        return jnp.maximum(high, jnp.max(product, axis=0))

    peak1[0] = lax.fori_loop(0, rows // top_rows, peak_step, high)

    def peak_copy(ref, k, to, phase):
        return pltpu.make_async_remote_copy(
            src_ref=ref.at[0],
            dst_ref=ref.at[k],
            send_sem=peak_send.at[phase],
            recv_sem=peak_recv.at[phase],
            device_id=to,
            device_id_type=MESH,
        )

    more = 2 * has_low.astype(jnp.int32) + 2 * has_high.astype(jnp.int32)
    pl.semaphore_wait(barrier, inner + outer - 2 + more)

    for k in range(1, inner):
        peak_copy(peak1, k, inner_id(k), 0).start()
    start_halo("x", "t", "m")
    first_force(chunks[1])
    wait("v", "e")
    start_halo("v", "e")
    first_force(chunks[2])
    mix_rows(*chunks[0])
    mix_rows(*chunks[1])
    wait_halo("x")
    pack(-1, edge)
    pack(pairs - edge + 1, edge)
    first_force(*edges)
    mix_rows(*chunks[2])
    wait_halo("t", "v")
    for first, n in edges:
        mix_rows(first, n)

    arrived1 = peak1.at[pl.ds(1, inner - 1)]
    pltpu.make_async_copy(arrived1, arrived1, peak_recv.at[0]).wait()
    peak2[0] = jnp.max(peak1[...], axis=0)
    for k in range(1, outer):
        peak_copy(peak2, k, outer_id(k), 1).start()

    pick_row = iota((COMPS * CODES, LANES), 0)
    pick_lane = iota((COMPS * CODES, LANES), 1)
    comp_of = pick_row // CODES
    code_of = pick_row % CODES
    picked = (pick_lane == comp_of * EDGE + code_of % EDGE) & (pick_lane < COMPS * EDGE)
    found = []
    for h in range(blocks):
        pick = jnp.where(picked & (code_of // EDGE == h), 1.0, 0.0).astype(BF16)
        found.append(dot_t(pick, mixm[pl.ds(h * LOW, LOW), :]))
    table[...] = (apart(p, sum(found[0::2])) + sum(found[1::2])).astype(BF16)

    def trace_copy(j):
        return pltpu.make_async_remote_copy(
            src_ref=sent.at[j],
            dst_ref=got.at[2 - j],
            send_sem=trace_send.at[j],
            recv_sem=trace_recv.at[2 - j],
            device_id={"grp": 1 - g, "patch": p + (j - 1)},
            device_id_type=MESH,
        )

    def guarded(cond, run):
        if cond is None:
            run()
        else:
            pl.when(cond)(run)

    code_id = iota((CODES, third), 0)

    for j in (0, 2, 1):
        result = jnp.zeros((SEG, third), F32)
        for q in range(3):
            found = dot(table[...], hot[j, :, parts[q]])
            mask = code_id == code_ref[pl.ds(j, 1), parts[q]]
            for c in range(COMPS):
                chosen = jnp.where(mask, found[c * CODES : (c + 1) * CODES], 0.0)
                result = jnp.where(
                    row16 == c * 3 + q, jnp.sum(chosen, axis=0, keepdims=True), result
                )
        own[j] = result
        sent[j] = result.astype(BF16)
    for j in (0, 2, 1):
        guarded(exists[j], lambda j=j: trace_copy(j).start())

    wait_halo("m", "e")

    def prepare(i, carry):
        for k in range(10):
            j = i * 10 + k
            at = (i * 5 + k // 2, k % 2)
            mass = rows_of(ms, seg_len, j)
            coef = mass * rows_of(ts, seg_len, j)
            applied = three(mass) * wide_rows_of(es, seg_len, j)
            ao[at] = applied
            co[at] = coef
            dd[at] = mass
            sbuf[at] = applied - three(coef) * sbuf[at]
            wo[at] = wide_rows_of(vs, seg_len, j)
            xo[at] = wide_rows_of(xs, seg_len, j)
        return carry

    lax.fori_loop(0, seg_len // 10, prepare, 0)

    for j in range(3):
        guarded(exists[j], lambda j=j: trace_copy(2 - j).wait_recv())
    zero = jnp.zeros((CODES, third), BF16)
    sums = []
    for j in range(3):
        value = (got[j].astype(F32) - own[j]) * wl[j]
        coarse = value.astype(BF16).astype(F32)
        fine = value - coarse
        for q in range(3):
            mask = code_id == code_ref[pl.ds(j, 1), parts[q]]
            stack = []
            for piece in (coarse, fine):
                for c in range(COMPS):
                    one = piece[c * 3 + q : c * 3 + q + 1]
                    stack.append(jnp.where(mask, one, 0.0).astype(BF16))
                stack.append(zero)
            sums.append(dot_t(hot[j, :, parts[q]], jnp.concatenate(stack, axis=0)))
    summed = apart(p, sum(sums[0::2])) + sum(sums[1::2])
    both = summed[:, :LANES] + summed[:, LANES:]
    acc[...] = both
    first = both.astype(BF16)
    pieces = jnp.concatenate([first, (both - first.astype(F32)).astype(BF16)], axis=1)

    fine_group = g == 1

    def edge_lane_rows(first_row):
        out = []
        for k in range(HALO):
            j = (first_row + k + BASE) % seg_len
            s = (first_row + k + BASE) // seg_len
            one = acc[pl.ds((j % SEG) * SEG + s, 1), :]
            keep = iota((1, LANES), 1) % CODES // EDGE == j // SEG
            out.append(jnp.where(keep, one, 0.0))
        return jnp.concatenate(out, axis=0)

    far_src[0] = edge_lane_rows(0)
    far_src[1] = edge_lane_rows(rows - HALO)

    def far_copy(up):
        return pltpu.make_async_remote_copy(
            src_ref=far_src.at[int(up)],
            dst_ref=far_dst.at[1 - int(up)],
            send_sem=far_send.at[int(up)],
            recv_sem=far_recv.at[int(up)],
            device_id={"grp": g, "patch": p + 1 if up else p - 1},
            device_id_type=MESH,
        )

    pl.when(jnp.logical_not(fine_group & has_low))(
        lambda: far_dst.at[0].__setitem__(..., jnp.zeros((HALO, LANES), F32))
    )
    pl.when(jnp.logical_not(fine_group & has_high))(
        lambda: far_dst.at[1].__setitem__(..., jnp.zeros((HALO, LANES), F32))
    )
    pl.when(fine_group & has_high)(lambda: far_copy(True).start())
    pl.when(fine_group & has_low)(lambda: far_copy(False).start())

    arrived2 = peak2.at[pl.ds(1, outer - 1)]
    pltpu.make_async_copy(arrived2, arrived2, peak_recv.at[1]).wait()
    top = jnp.max(jnp.max(peak2[...], axis=0), axis=(0, 1), keepdims=True)
    base_step = COURANT * (1.0 / jnp.sqrt(top))
    size = jnp.where(g == 0, SUBSTEPS * base_step, base_step)
    square = size * size
    half = SEG // 2

    def finish(h):
        n = min(half, pairs - h * half)
        placed = dot(pieces[: 2 * n * SEG], place[h]).reshape(n, 2, SEG, width)
        for k in range(n):
            for par in range(2):
                at = (h * half + k, par)
                extra = three(dd[at]) * placed[k, par]
                moved = size * wo[at] + square * (sbuf[at] + extra)
                there = xo[at] + moved
                ao[at] = square * (ao[at] + extra)
                co[at] = square * co[at]
                wo[at] = moved
                xo[at] = there
                xb1[at[0] + 1, par] = there.astype(BF16)

    @pl.when(g == 0)
    def _():
        for h in range(blocks):
            finish(h)

    @pl.when(fine_group)
    def _():
        def sums_of(k):
            return pair_force(xb1, band, band_mid, chunks[k])

        def step_of(k, sums):
            advance(sums, (xo, wo), (xo, wo), ao, co, xb2, chunks[k])

        bounds = [(first + n) // half + 1 for first, n in chunks]
        for h in range(1, bounds[0]):
            finish(h)
        sums = sums_of(0)
        for h in range(bounds[0], bounds[1]):
            finish(h)
        step_of(0, sums)
        sums = sums_of(1)
        for h in [*range(bounds[1], blocks), 0]:
            finish(h)
        step_of(1, sums)
        pl.when(has_low)(lambda: far_copy(True).wait_recv())
        pl.when(has_high)(lambda: far_copy(False).wait_recv())
        sums = sums_of(2)
        any_place = place[0]
        for h in range(1, blocks):
            any_place = any_place + place[h]
        far = far_dst[...].reshape(2 * HALO, LANES)
        far_first = far.astype(BF16)
        far_pieces = jnp.concatenate([far_first, (far - far_first.astype(F32)).astype(BF16)], axis=1)
        far_placed = dot(far_pieces, any_place)
        seg_id = iota((SEG, width), 0)
        for side, first_row in ((0, -HALO), (1, rows)):
            for k in range(HALO):
                j = (first_row + k + BASE) % seg_len
                s = (first_row + k + BASE) // seg_len
                at = (j // 2, j % 2)
                one = far_placed[side * HALO + k : side * HALO + k + 1]
                extra = square * three(dd[at]) * jnp.where(seg_id == s, one, 0.0)
                there = xo[at] + extra
                ao[at] = ao[at] + extra
                wo[at] = wo[at] + extra
                xo[at] = there
                xb1[at[0] + 1, at[1]] = there.astype(BF16)
        step_of(2, sums)

    for par in range(2):
        xb1[0, par] = pltpu.roll(xo[pairs - 1, par], 1, 0).astype(BF16)
        xb1[pairs + 1, par] = pltpu.roll(xo[0, par], SEG - 1, 0).astype(BF16)
    size_out[...] = jnp.broadcast_to(1.0 / size, size_out.shape)

    @pl.when(has_high)
    def _():
        for name in "xtvme":
            for copy in halo_copies(name, True):
                copy.wait_send()

    @pl.when(has_low)
    def _():
        for name in "xtvme":
            for copy in halo_copies(name, False):
                copy.wait_send()

    for j in range(3):
        guarded(exists[j], lambda j=j: trace_copy(j).wait_send())
    pl.when(fine_group & has_high)(lambda: far_copy(True).wait_send())
    pl.when(fine_group & has_low)(lambda: far_copy(False).wait_send())
    pltpu.make_async_copy(arrived1, arrived1, peak_send.at[0]).wait()
    pltpu.make_async_copy(arrived2, arrived2, peak_send.at[1]).wait()


def steps_kernel(
    x1, w1, a, c, xb1, mids, band, band_mid, inverse, disp_out, vel_out, xo, wo, xb2, xb3, xs, vs, out_sem
):
    g = lax.axis_index("grp")
    rows = disp_out.shape[1]
    width = disp_out.shape[2]
    total = rows + 2 * BASE
    seg_len = total // SEG
    pairs = seg_len // 2
    scale = inverse[0:1, 0:1]

    def put(i, par, x, w):
        j = 2 * i + par
        v = w * scale
        for value, ref in ((x, xs), (v, vs)):
            for c in range(COMPS):
                for half in range(2):
                    at = pl.ds(OFF + j + half * 8 * seg_len, 8, stride=seg_len)
                    ref[c, at, :] = value[half * 8 : half * 8 + 8, c * LANES : (c + 1) * LANES]

    def whole():
        copies = []
        for k, (ref, out) in enumerate(((xs, disp_out), (vs, vel_out))):
            for c in range(COMPS):
                copies.append(
                    pltpu.make_async_copy(
                        ref.at[c, pl.ds(OFF + BASE, rows)],
                        out.at[0, :, pl.ds(c * LANES, LANES)],
                        out_sem.at[k, c],
                    )
                )
        return copies

    def drain():
        copies = whole()
        for copy in copies:
            copy.start()
        for copy in copies:
            copy.wait()

    def pieces(bounds):
        copies = []
        for k, (ref, out) in enumerate(((xs, disp_out), (vs, vel_out))):
            for lo, hi in bounds:
                for c in range(COMPS):
                    copies.append(
                        pltpu.make_async_copy(
                            ref.at[c, pl.ds(OFF + BASE + lo, hi - lo)],
                            out.at[0, pl.ds(lo, hi - lo), pl.ds(c * LANES, LANES)],
                            out_sem.at[k, c],
                        )
                    )
        return copies

    @pl.when(g == 0)
    def _():
        def move(i, carry):
            for par in range(2):
                put(i, par, x1[i, par], w1[i, par])
            return carry

        lax.fori_loop(0, pairs, move, 0)
        drain()

    @pl.when(g == 1)
    def _():
        _, chunks, edges = row_ranges(pairs)
        order = [[chunks[1]], [chunks[0]], [chunks[2]], edges]
        middle = pl.ds(chunks[0][0] + 1, sum(n for _, n in chunks))

        def wrap(nxt):
            for par in range(2):
                nxt[0, par] = pltpu.roll(xo[pairs - 1, par], 1, 0).astype(BF16)
                nxt[pairs + 1, par] = pltpu.roll(xo[0, par], SEG - 1, 0).astype(BF16)

        def first_step(sums, ranges):
            advance(sums, (x1, w1), (xo, wo), a, c, xb2, *ranges)
            wrap(xb2)

        def second_step(sums, ranges):
            src = (xo, wo) if ranges is edges else (x1, w1)
            advance(sums, src, (xo, wo), a, c, xb3, *ranges)
            if ranges is edges:
                wrap(xb3)

        def third_step(sums, ranges):
            done = 0
            for first, n in ranges:
                for i in range(n):
                    for par in range(2):
                        at = (first + i, par)
                        w = wo[at] + a[at] - three(c[at]) * sums[par][done + i]
                        put(first + i, par, xo[at] + w, w)
                done += n

        tasks = [(first_step, xb1, edges)]
        tasks += [(second_step, xb2, ranges) for ranges in order]
        tasks += [(third_step, xb3, ranges) for ranges in order]
        xb2[middle] = mids[middle]
        inner = []
        begin, end = 2 * chunks[0][0], 2 * (chunks[-1][0] + chunks[-1][1])
        for s in range(SEG):
            lo = -(-(s * seg_len + begin - BASE) // 8) * 8
            hi = (s * seg_len + end - BASE) // 8 * 8
            inner.append((max(lo, 0), min(hi, rows)))
        outer = [(lo, hi) for lo, hi in zip([0] + [hi for _, hi in inner], [lo for lo, _ in inner] + [rows]) if hi > lo]
        last = None
        for task, cur, ranges in tasks:
            sums = pair_force(cur, band, band_mid, *ranges)
            if last is not None:
                last[0](*last[1:])
            last = (task, sums, ranges)
        for copy in pieces(inner):
            copy.start()
        last[0](*last[1:])
        for copy in pieces(outer):
            copy.start()
        for copy in whole():
            copy.wait()


def per_device(
    n_grp,
    n_patch,
    displace,
    velocity,
    ext_force,
    inv_mass,
    thickness,
    stiff_bands,
    pair_points,
    pair_weights,
):
    rows, width = displace.shape[1:]
    slots = pair_points.shape[3]
    total = rows + 2 * BASE
    seg_len = total // SEG
    pairs = seg_len // 2
    blocks = -(-seg_len // SEG)
    third = slots // 3
    taps = stiff_bands.shape[0]
    bands = stiff_bands.reshape(taps * width, width)
    points = pair_points.reshape(3, 1, slots)
    weights = pair_weights.reshape(3, 1, slots)
    hbm = pl.BlockSpec(memory_space=pltpu.HBM)
    vmem = pl.BlockSpec(memory_space=pltpu.VMEM)
    dma = pltpu.SemaphoreType.DMA
    lined = total + 2 * OFF
    wide = pltpu.VMEM((COMPS, lined, LANES), F32)
    slim = pltpu.VMEM((lined, LANES), F32)
    seg_wide = pltpu.VMEM((pairs, 2, SEG, width), F32)
    seg_slim = pltpu.VMEM((pairs, 2, SEG, LANES), F32)
    seg_bf16 = pltpu.VMEM((pairs + 2, 2, SEG, width), BF16)
    state = pl.pallas_call(
        functools.partial(kernel, n_grp, n_patch),
        out_shape=[
            seg_wide,
            seg_wide,
            seg_wide,
            seg_slim,
            seg_bf16,
            seg_bf16,
            pltpu.VMEM(bands.shape, BF16),
            pltpu.VMEM(((taps + 1) * width, 2 * LANES), BF16),
            pltpu.VMEM((8, LANES), F32),
        ],
        in_specs=[hbm] * 8,
        out_specs=[vmem] * 9,
        scratch_shapes=[
            wide,
            wide,
            wide,
            slim,
            slim,
            seg_bf16,
            seg_wide,
            seg_slim,
            pltpu.VMEM((blocks * LOW, LANES), BF16),
            pltpu.VMEM((COMPS * CODES, LOW), BF16),
            pltpu.VMEM((3, LOW, slots), BF16),
            pltpu.VMEM((blocks, LOW, width), BF16),
            pltpu.VMEM((3, 1, slots), jnp.int32),
            pltpu.VMEM((3, slots), jnp.int32),
            pltpu.VMEM((3, 1, slots), F32),
            pltpu.VMEM((3, slots), jnp.int32),
            pltpu.VMEM((3, SEG, third), F32),
            pltpu.VMEM((3, SEG, third), F32),
            pltpu.VMEM((3, SEG, third), BF16),
            pltpu.VMEM((3, SEG, third), BF16),
            pltpu.VMEM((LOW, LANES), F32),
            pltpu.VMEM((2, HALO, LANES), F32),
            pltpu.VMEM((2, HALO, LANES), F32),
            pltpu.VMEM((n_grp * INNER, 8, LANES), F32),
            pltpu.VMEM((n_patch // INNER, 8, LANES), F32),
            dma((16,)),
            dma((11, 2)),
            dma((11, 2)),
            dma((3,)),
            dma((3,)),
            dma((2,)),
            dma((2,)),
            dma((2,)),
            dma((2,)),
        ],
        compiler_params=pltpu.CompilerParams(
            has_side_effects=True, collective_id=0, vmem_limit_bytes=44 * 1024 * 1024
        ),
        name="couple_step",
    )(displace, velocity, ext_force, inv_mass, thickness, bands, points, weights)
    return pl.pallas_call(
        steps_kernel,
        out_shape=[jax.ShapeDtypeStruct(displace.shape, F32)] * 2,
        in_specs=[vmem] * 9,
        out_specs=[hbm] * 2,
        scratch_shapes=[seg_wide, seg_wide, seg_bf16, seg_bf16, wide, wide, dma((2, COMPS))],
        compiler_params=pltpu.CompilerParams(vmem_limit_bytes=20 * 1024 * 1024),
        name="fine_steps",
    )(*state)


def solution(mesh):
    return jax.shard_map(
        functools.partial(per_device, mesh.shape["grp"], mesh.shape["patch"]),
        mesh=mesh,
        in_specs=(
            P("grp", "patch", None),
            P("grp", "patch", None),
            P("grp", "patch", None),
            P("grp", "patch", None),
            P("grp", "patch", None),
            P(),
            P("grp", "patch", None, None),
            P("grp", "patch", None, None),
        ),
        out_specs=(P("grp", "patch", None), P("grp", "patch", None)),
        check_vma=False,
    )
```
